32 devices in a mesh: dp: 1 (over z), ep: 32 (over y, x, core).
Axes of the slice: x: 4, y: 4, z: 1, core: 2. Of those that a mesh axis runs over, the one named last changes fastest.
The devices are a block of a 4x4x8 slice.
Arguments:
- x_tok: bfloat16 [16384, 2048], P(('dp', 'ep'))
- topk_idx: int32 [16384, 6], P(('dp', 'ep'))
- topk_w: float32 [16384, 6], P(('dp', 'ep'))
- w_in: bfloat16 [64, 2048, 1408], P('ep')
- w_out: bfloat16 [64, 1408, 2048], P('ep')
- shared_in: bfloat16 [2048, 2816], replicated
- shared_out: bfloat16 [2816, 2048], replicated
Outputs:
- output: bfloat16 [16384, 2048], P(('dp', 'ep'))
All inputs are finite; a program needn't handle non-finite values.
Results may differ from the reference program's by a relative error of at most 0.001.
Values are sent between devices in bfloat16 or wider.
A program may use at most 768 MiB of HBM per device.

```python
import jax
import jax.numpy as jnp
from jax import lax

GROUP_SIZE = 32
TOK_DEV = 512
D_MODEL = 2048
FF_DIM = 1408
FS_DIM = 2816
EXPERTS = 64
TOP_K = 6
NUM_HOT = 2
SLOT_CAP = 144

TOKENS = GROUP_SIZE * TOK_DEV
EXPERT_ROWS = SLOT_CAP * GROUP_SIZE


def draw_routing(route_key):
    key_hot, key_extra, key_tok, key_rot = jax.random.split(route_key, 4)
    cold_count = EXPERTS - NUM_HOT
    rest_pairs = TOK_DEV * TOP_K - NUM_HOT * SLOT_CAP
    base_load = rest_pairs // cold_count
    extra_pairs = rest_pairs - base_load * cold_count
    expert_order = jax.random.permutation(key_hot, EXPERTS)
    cold_rank = jax.vmap(lambda dev_key: jax.random.permutation(dev_key, cold_count))(jax.random.split(key_extra, GROUP_SIZE))
    cold_load = base_load + (cold_rank < extra_pairs).astype(jnp.int32)
    hot_load = jnp.full((GROUP_SIZE, NUM_HOT), SLOT_CAP, jnp.int32)
    ordered_load = jnp.concatenate([hot_load, cold_load], axis=1)
    expert_load = jnp.zeros((GROUP_SIZE, EXPERTS), jnp.int32).at[:, expert_order].set(ordered_load)
    load_ends = jnp.cumsum(expert_load, axis=1)
    pair_ids = jnp.arange(TOK_DEV * TOP_K, dtype=jnp.int32)
    pair_expert = jax.vmap(lambda ends_row: jnp.searchsorted(ends_row, pair_ids, side='right'))(load_ends)
    slot_table = pair_expert.reshape(GROUP_SIZE, TOP_K, TOK_DEV).transpose(0, 2, 1)
    tok_perm = jax.vmap(lambda dev_key: jax.random.permutation(dev_key, TOK_DEV))(jax.random.split(key_tok, GROUP_SIZE))
    tok_index = jnp.broadcast_to(tok_perm[:, :, None], (GROUP_SIZE, TOK_DEV, TOP_K))
    slot_table = jnp.take_along_axis(slot_table, tok_index, axis=1)
    slot_shift = jax.random.randint(key_rot, (GROUP_SIZE, TOK_DEV, 1), 0, TOP_K)
    slot_cols = (jnp.arange(TOP_K)[None, None, :] + slot_shift) % TOP_K
    slot_table = jnp.take_along_axis(slot_table, slot_cols, axis=2)
    return slot_table.reshape(TOKENS, TOP_K).astype(jnp.int32)


def draw_stack(stack_key, fan_in, fan_out):
    def one_expert(expert_key):
        return (jax.random.normal(expert_key, (fan_in, fan_out), jnp.float32) * fan_in ** -0.5).astype(jnp.bfloat16)
    return lax.map(one_expert, jax.random.split(stack_key, EXPERTS))


def setup_inputs(seed: int = 0, part: int = 0) -> dict:
    root_key = jax.random.key(seed)
    key_x, key_route, key_gate, key_in, key_out, key_sin, key_sout = jax.random.split(root_key, 7)
    x_tok = jax.random.normal(jax.random.fold_in(key_x, part), (TOKENS, D_MODEL), jnp.float32).astype(jnp.bfloat16)
    topk_idx = draw_routing(jax.random.fold_in(key_route, part))
    gate_raw = jax.random.uniform(jax.random.fold_in(key_gate, part), (TOKENS, TOP_K), jnp.float32, 0.2, 1.0)
    topk_w = gate_raw * (1.5 / TOP_K ** 0.5)
    w_in = draw_stack(key_in, D_MODEL, FF_DIM)
    w_out = draw_stack(key_out, FF_DIM, D_MODEL)
    shared_in = (jax.random.normal(key_sin, (D_MODEL, FS_DIM), jnp.float32) * D_MODEL ** -0.5).astype(jnp.bfloat16)
    shared_out = (jax.random.normal(key_sout, (FS_DIM, D_MODEL), jnp.float32) * FS_DIM ** -0.5).astype(jnp.bfloat16)
    return {'x_tok': x_tok, 'topk_idx': topk_idx, 'topk_w': topk_w, 'w_in': w_in, 'w_out': w_out, 'shared_in': shared_in, 'shared_out': shared_out}


def reference(x_tok, topk_idx, topk_w, w_in, w_out, shared_in, shared_out):
    pair_total = TOKENS * TOP_K
    flat_ids = topk_idx.reshape(pair_total)
    pair_order = jnp.argsort(flat_ids, stable=True)
    counts = jnp.zeros((EXPERTS,), jnp.int32).at[flat_ids].add(1)
    starts = jnp.cumsum(counts) - counts
    pair_gates = topk_w.astype(jnp.bfloat16).astype(jnp.float32).reshape(pair_total)
    slot_ids = jnp.arange(EXPERT_ROWS)

    def expert_step(routed_acc, step_in):
        e_index, w_first, w_second = step_in
        slot_valid = slot_ids < counts[e_index]
        pair_pos = pair_order[jnp.minimum(starts[e_index] + slot_ids, pair_total - 1)]
        tok_pos = pair_pos // TOP_K
        gathered = x_tok[tok_pos]
        hidden = jax.nn.gelu(jnp.dot(gathered, w_first, preferred_element_type=jnp.float32), approximate=True).astype(jnp.bfloat16)
        expert_out = jnp.dot(hidden, w_second, preferred_element_type=jnp.float32).astype(jnp.bfloat16)
        pair_scale = jnp.where(slot_valid, pair_gates[pair_pos], 0.0)
        contrib = expert_out.astype(jnp.float32) * pair_scale[:, None]
        return routed_acc.at[tok_pos].add(contrib), None

    routed_init = jnp.zeros((TOKENS, D_MODEL), jnp.float32)
    routed, _ = lax.scan(expert_step, routed_init, (jnp.arange(EXPERTS), w_in, w_out))
    shared_hidden = jax.nn.gelu(jnp.dot(x_tok, shared_in, preferred_element_type=jnp.float32), approximate=True).astype(jnp.bfloat16)
    shared_val = jnp.dot(shared_hidden, shared_out, preferred_element_type=jnp.float32)
    return (routed + shared_val).astype(jnp.bfloat16)
```

```python
import functools

import jax
import jax.numpy as jnp
from jax import lax
from jax.experimental import pallas as pl
from jax.experimental.pallas import tpu as pltpu
from jax.sharding import PartitionSpec as P

LOAD_MULT = 3
BASE_CAP = 48
HOT_STATIC = 2
SRC_BLOCK = 8


def gelu(z):
    return jax.nn.gelu(z, approximate=True)


def gather_rows(slot_ref, x_ref, rows_ref, cap):
    groups, blk, toks = slot_ref.shape
    slot_iota = lax.broadcasted_iota(jnp.int32, (cap, toks), 0)

    def one(s, carry):
        picks = [(slot_iota == slot_ref[g, pl.ds(s, 1), :]).astype(jnp.bfloat16) for g in range(groups)]
        pick = jnp.concatenate(picks, axis=0)
        got = jnp.dot(pick, x_ref[s], preferred_element_type=jnp.float32).astype(jnp.bfloat16)
        for g in range(groups):
            rows_ref[g, pl.ds(pl.multiple_of(s * cap, 16), cap), :] = got[g * cap:(g + 1) * cap]
        return carry

    lax.fori_loop(0, blk, one, 0)


def first_kernel(cap, wsel_ref, slot_ref, x_ref, w0_ref, w1_ref, acc_ref, rows_ref):
    gather_rows(slot_ref, x_ref, rows_ref, cap)
    for g, w_ref in enumerate((w0_ref, w1_ref)):
        acc_ref[g] = jnp.dot(rows_ref[g], w_ref[0], preferred_element_type=jnp.float32)


def second_kernel(cap, wsel_ref, slot_ref, x_ref, acc_ref, w0_ref, w1_ref, v0_ref, v1_ref, out_ref, rows_ref):
    blk = x_ref.shape[0]
    gather_rows(slot_ref, x_ref, rows_ref, cap)
    for g, (w_ref, v_ref) in enumerate(((w0_ref, v0_ref), (w1_ref, v1_ref))):
        pre = acc_ref[g] + jnp.dot(rows_ref[g], w_ref[0], preferred_element_type=jnp.float32)
        hid = gelu(pre).astype(jnp.bfloat16)
        out = jnp.dot(hid, v_ref[0], preferred_element_type=jnp.float32).astype(jnp.bfloat16)
        out_ref[:, g] = out.reshape(blk, cap, out.shape[-1])


def first_half(wsel, slots, x_part, w_in, cap):
    groups, srcs, toks = slots.shape
    width = x_part.shape[2]
    ff = w_in.shape[2]
    blk = SRC_BLOCK
    wspec = lambda g: pl.BlockSpec((1, width, ff), lambda i, w: (w[g], 0, 0), pipeline_mode=pl.Buffered(1))
    return pl.pallas_call(
        functools.partial(first_kernel, cap),
        out_shape=jax.ShapeDtypeStruct((groups, srcs * cap, ff), jnp.float32),
        grid_spec=pltpu.PrefetchScalarGridSpec(
            num_scalar_prefetch=1,
            grid=(srcs // blk,),
            in_specs=[
                pl.BlockSpec((groups, blk, toks), lambda i, w: (0, i, 0)),
                pl.BlockSpec((blk, toks, width), lambda i, w: (i, 0, 0)),
                wspec(0), wspec(1),
            ],
            out_specs=pl.BlockSpec((groups, blk * cap, ff), lambda i, w: (0, i, 0)),
            scratch_shapes=[pltpu.VMEM((groups, blk * cap, width), jnp.bfloat16)],
        ),
        compiler_params=pltpu.CompilerParams(dimension_semantics=("arbitrary",), vmem_limit_bytes=60 * 2 ** 20),
        cost_estimate=pl.CostEstimate(
            flops=2 * groups * srcs * cap * width * (ff + toks),
            bytes_accessed=x_part.size * 2 + groups * (width * ff * 2 + srcs * cap * ff * 4), transcendentals=0),
        name="expert_first",
    )(wsel, slots, x_part, w_in, w_in)


def second_half(wsel, slots, x_part, acc, w_in, w_out, cap):
    groups, srcs, toks = slots.shape
    width = x_part.shape[2]
    ff, model = w_out.shape[1:]
    blk = SRC_BLOCK
    wspec = lambda g: pl.BlockSpec((1, width, ff), lambda i, w: (w[g], 1, 0), pipeline_mode=pl.Buffered(1))
    vspec = lambda g: pl.BlockSpec((1, ff, model), lambda i, w: (w[g], 0, 0), pipeline_mode=pl.Buffered(1))
    return pl.pallas_call(
        functools.partial(second_kernel, cap),
        out_shape=jax.ShapeDtypeStruct((srcs, groups, cap, model), jnp.bfloat16),
        grid_spec=pltpu.PrefetchScalarGridSpec(
            num_scalar_prefetch=1,
            grid=(srcs // blk,),
            in_specs=[
                pl.BlockSpec((groups, blk, toks), lambda i, w: (0, i, 0)),
                pl.BlockSpec((blk, toks, width), lambda i, w: (i, 0, 0)),
                pl.BlockSpec((groups, blk * cap, ff), lambda i, w: (0, i, 0)),
                wspec(0), wspec(1), vspec(0), vspec(1),
            ],
            out_specs=pl.BlockSpec((blk, groups, cap, model), lambda i, w: (i, 0, 0, 0)),
            scratch_shapes=[pltpu.VMEM((groups, blk * cap, width), jnp.bfloat16)],
        ),
        compiler_params=pltpu.CompilerParams(dimension_semantics=("arbitrary",), vmem_limit_bytes=62 * 2 ** 20),
        cost_estimate=pl.CostEstimate(
            flops=2 * groups * srcs * cap * (width * (ff + toks) + ff * model),
            bytes_accessed=x_part.size * 2 + groups * (width * ff * 2 + ff * model * 2 + srcs * cap * (ff * 4 + model * 2)),
            transcendentals=groups * srcs * cap * ff),
        name="expert_second",
    )(wsel, slots, x_part, acc, w_in, w_in, w_out, w_out)


def solution(mesh):
    group_size = mesh.shape['ep']

    def local_layer(x_loc, idx_loc, gate_loc, w_in, w_out, shared_in, shared_out):
        tok_rows, top_k = idx_loc.shape
        model = x_loc.shape[1]
        own = w_in.shape[0]
        num_experts = own * group_size
        slot_cap = min(tok_rows, LOAD_MULT * tok_rows * top_k // num_experts)
        cap = BASE_CAP
        over_cap = slot_cap - cap
        half = model // 2
        me = lax.axis_index('ep')

        before = (lax.broadcasted_iota(jnp.int32, (tok_rows, tok_rows), 0)
                  <= lax.broadcasted_iota(jnp.int32, (tok_rows, tok_rows), 1)).astype(jnp.bfloat16)

        def slots_of(hit):
            count = jnp.dot(hit.reshape(-1, tok_rows).astype(jnp.bfloat16), before, preferred_element_type=jnp.float32)
            return jnp.where(hit, count.reshape(hit.shape).astype(jnp.int32) - 1, -1)

        idx_t = idx_loc.T
        gate_t = gate_loc.astype(jnp.bfloat16).T
        same = idx_t[None] == jnp.arange(num_experts, dtype=jnp.int32)[:, None, None]
        hit_loc = jnp.any(same, axis=1)
        gate_of = jnp.sum(jnp.where(same, gate_t[None], 0).astype(jnp.float32), axis=1).astype(jnp.bfloat16)
        slot_loc = slots_of(hit_loc)
        count_loc = jnp.max(slot_loc, axis=1) + 1

        counts_row = jnp.zeros((1, tok_rows), jnp.int32).at[0, :num_experts].set(count_loc)
        table = jnp.concatenate([idx_t, counts_row, jnp.full((16 - top_k - 1, tok_rows), -1, jnp.int32)], axis=0)
        tables = lax.all_gather(table, 'ep')
        x_first = lax.all_gather(x_loc[:, :half], 'ep')
        x_second = lax.all_gather(x_loc[:, half:], 'ep')
        idx_all = tables[:, :top_k]
        load = jnp.max(tables[:, top_k, :num_experts], axis=0)

        over = load > cap
        over_rank = jnp.cumsum(over.astype(jnp.int32)) - 1
        num_over = jnp.sum(over.astype(jnp.int32))

        def over_expert(i):
            chosen = over & (over_rank == i)
            return jnp.where(i < num_over, jnp.sum(jnp.where(chosen, jnp.arange(num_experts, dtype=jnp.int32), 0)), num_experts)

        def slots_all(expert):
            return slots_of(jnp.any(idx_all == expert, axis=1))

        shared_hidden = gelu(jnp.dot(x_loc, shared_in, preferred_element_type=jnp.float32)).astype(jnp.bfloat16)
        shared_val = jnp.dot(shared_hidden, shared_out, preferred_element_type=jnp.float32)

        base_sel = jnp.arange(own, dtype=jnp.int32)
        base_slots = jnp.stack([slots_all(me * own + g) for g in range(own)])

        def over_setup(i):
            expert = over_expert(i)
            mine = expert // own == me
            sel = jnp.where(mine, expert % own, 0) * jnp.ones((2,), jnp.int32)
            slots = slots_all(expert) - cap
            return expert, mine, sel, jnp.stack([slots, slots - over_cap // 2])

        def over_first(setup, x_part):
            expert, mine, sel, slots = setup
            return lax.cond(
                mine, lambda: first_half(sel, slots, x_part, w_in, over_cap // 2),
                lambda: jnp.zeros((2, group_size * over_cap // 2, w_in.shape[2]), jnp.float32))

        def over_second(setup, x_part, acc):
            expert, mine, sel, slots = setup
            out = lax.cond(
                mine, lambda: second_half(sel, slots, x_part, acc, w_in, w_out, over_cap // 2),
                lambda: jnp.zeros((group_size, 2, over_cap // 2, model), jnp.bfloat16))
            return lax.psum_scatter(out.reshape(group_size * over_cap, model), 'ep', scatter_dimension=0, tiled=True)

        def over_combine(setup, rows):
            expert = setup[0]
            slot = lax.dynamic_index_in_dim(slot_loc, jnp.minimum(expert, num_experts - 1), 0, keepdims=True)
            gate = lax.dynamic_index_in_dim(gate_of, jnp.minimum(expert, num_experts - 1), 0, keepdims=True)
            pick = (slot - cap == lax.broadcasted_iota(jnp.int32, (over_cap, tok_rows), 0)) & (expert < num_experts)
            comb = jnp.where(pick, gate, 0).astype(jnp.bfloat16)
            return lax.dot_general(comb, rows, (((0,), (0,)), ((), ())), preferred_element_type=jnp.float32)

        setups = [over_setup(i) for i in range(HOT_STATIC)]
        accs = [over_first(setup, x_first) for setup in setups]
        base_acc = first_half(base_sel, base_slots, x_first, w_in, cap)
        accs, base_acc, x_second = lax.optimization_barrier((accs, base_acc, x_second))
        over_rows = [over_second(setup, x_second, acc) for setup, acc in zip(setups, accs)]
        base_out = second_half(base_sel, base_slots, x_second, base_acc, w_in, w_out, cap)
        back = lax.all_to_all(base_out.reshape(group_size, own * cap, model), 'ep', 0, 0, tiled=True)

        pick = slot_loc[:, None, :] == jnp.arange(cap, dtype=jnp.int32)[None, :, None]
        comb = jnp.where(pick, gate_of[:, None, :], 0).astype(jnp.bfloat16).reshape(num_experts * cap, tok_rows)
        routed = lax.dot_general(comb, back.reshape(num_experts * cap, model), (((0,), (0,)), ((), ())), preferred_element_type=jnp.float32)
        total = routed + shared_val
        for setup, rows in zip(setups, over_rows):
            total = total + over_combine(setup, rows)

        def more(i, total):
            setup = over_setup(i)
            rows = over_second(setup, x_second, over_first(setup, x_first))
            return total + over_combine(setup, rows)

        total = lax.fori_loop(HOT_STATIC, jnp.maximum(num_over, HOT_STATIC), more, total)
        return total.astype(jnp.bfloat16)

    tok_spec = P(('dp', 'ep'), None)
    expert_spec = P('ep', None, None)
    whole_spec = P(None, None)
    return jax.shard_map(local_layer, mesh=mesh, in_specs=(tok_spec, tok_spec, tok_spec, expert_spec, expert_spec, whole_spec, whole_spec), out_specs=tok_spec, check_vma=False)
```

```python
import functools

import jax
import jax.numpy as jnp
from jax import lax
from jax.experimental import pallas as pl
from jax.experimental.pallas import tpu as pltpu
from jax.sharding import PartitionSpec as P

LOAD_MULT = 3
BASE_CAP = 48
HOT_STATIC = 2
SRC_BLOCK = 8
OVER_BLOCK = 4
EXTRA_ROWS = 16
VMEM = 60 * 2 ** 20


def gelu(z):
    return jax.nn.gelu(z, approximate=True)


def gather_rows(slot_ref, x_ref, cap, put):
    groups, blk, toks = slot_ref.shape
    slot_iota = lax.broadcasted_iota(jnp.int32, (cap, toks), 0)

    def one(s, carry):
        picks = [(slot_iota == slot_ref[g, pl.ds(s, 1), :]).astype(jnp.bfloat16) for g in range(groups)]
        pick = jnp.concatenate(picks, axis=0) if groups > 1 else picks[0]
        got = jnp.dot(pick, x_ref[s], preferred_element_type=jnp.float32).astype(jnp.bfloat16)
        for g in range(groups):
            put(g, pl.ds(pl.multiple_of(s * cap, 16), cap), got[g * cap:(g + 1) * cap])
        return carry

    lax.fori_loop(0, blk, one, 0)


def first_kernel(cap, slot_ref, x_ref, w_ref, acc_ref, rows_ref):
    def put(g, where, rows):
        rows_ref[g, where, :] = rows

    gather_rows(slot_ref, x_ref, cap, put)
    for g in range(w_ref.shape[0]):
        acc_ref[g] = jnp.dot(rows_ref[g], w_ref[g], preferred_element_type=jnp.float32)


def finish(cap, rows, acc_ref, w_ref, v_ref, out_ref):
    pre = acc_ref[0] + jnp.dot(rows, w_ref[0], preferred_element_type=jnp.float32)
    hid = gelu(pre).astype(jnp.bfloat16)
    out = jnp.dot(hid, v_ref[0], preferred_element_type=jnp.float32).astype(jnp.bfloat16)
    out_ref[...] = out.reshape(out_ref.shape)


def second_kernel(cap, slot_ref, x_ref, acc_ref, w_ref, v_ref, out_ref, rest_ref, rows_ref):
    def put(g, where, rows):
        if g == 0:
            rows_ref[where, :] = rows
        else:
            rest_ref[g - 1, where, :] = rows

    gather_rows(slot_ref, x_ref, cap, put)
    finish(cap, rows_ref[...], acc_ref, w_ref, v_ref, out_ref)


def third_kernel(cap, rows_ref, acc_ref, w_ref, v_ref, out_ref):
    finish(cap, rows_ref[0], acc_ref, w_ref, v_ref, out_ref)


def over_kernel(cap, sel_ref, slot_ref, xa_ref, xb_ref, w_ref, v_ref, out_ref, rows_ref):
    width = xa_ref.shape[2]

    def put_a(g, where, rows):
        rows_ref[where, :width] = rows

    def put_b(g, where, rows):
        rows_ref[where, width:] = rows

    gather_rows(slot_ref, xa_ref, cap, put_a)
    gather_rows(slot_ref, xb_ref, cap, put_b)
    hid = gelu(jnp.dot(rows_ref[...], w_ref[0], preferred_element_type=jnp.float32)).astype(jnp.bfloat16)
    out = jnp.dot(hid, v_ref[0], preferred_element_type=jnp.float32).astype(jnp.bfloat16)
    out_ref[...] = out.reshape(out_ref.shape)


def params():
    return pltpu.CompilerParams(dimension_semantics=("arbitrary",), vmem_limit_bytes=VMEM)


def cost(flops, nbytes, trans=0):
    return pl.CostEstimate(flops=int(flops), bytes_accessed=int(nbytes), transcendentals=int(trans))


def once(shape, index):
    return pl.BlockSpec(shape, index, pipeline_mode=pl.Buffered(1))


def base_first(slots, x_part, w_in, cap):
    groups, srcs, toks = slots.shape
    width, ff, blk = x_part.shape[2], w_in.shape[2], SRC_BLOCK
    return pl.pallas_call(
        functools.partial(first_kernel, cap),
        out_shape=jax.ShapeDtypeStruct((groups, srcs * cap, ff), jnp.float32),
        grid=(srcs // blk,),
        in_specs=[
            pl.BlockSpec((groups, blk, toks), lambda i: (0, i, 0)),
            pl.BlockSpec((blk, toks, width), lambda i: (i, 0, 0)),
            once((groups, width, ff), lambda i: (0, 0, 0)),
        ],
        out_specs=pl.BlockSpec((groups, blk * cap, ff), lambda i: (0, i, 0)),
        scratch_shapes=[pltpu.VMEM((groups, blk * cap, width), jnp.bfloat16)],
        compiler_params=params(),
        cost_estimate=cost(2 * groups * srcs * cap * width * (ff + toks),
                           srcs * toks * width * 2 + groups * (width * ff * 2 + srcs * cap * ff * 4)),
        name="expert_first",
    )(slots, x_part, w_in)


def base_second(slots, x_part, acc, w_in, w_out, cap):
    groups, srcs, toks = slots.shape
    width, ff, model, blk = x_part.shape[2], w_out.shape[1], w_out.shape[2], SRC_BLOCK
    last = w_in.shape[1] // width - 1
    return pl.pallas_call(
        functools.partial(second_kernel, cap),
        out_shape=(jax.ShapeDtypeStruct((srcs, cap, model), jnp.bfloat16),
                   jax.ShapeDtypeStruct((groups - 1, srcs * cap, width), jnp.bfloat16)),
        grid=(srcs // blk,),
        in_specs=[
            pl.BlockSpec((groups, blk, toks), lambda i: (0, i, 0)),
            pl.BlockSpec((blk, toks, width), lambda i: (i, 0, 0)),
            pl.BlockSpec((1, blk * cap, ff), lambda i: (0, i, 0)),
            once((1, width, ff), lambda i: (0, last, 0)),
            once((1, ff, model), lambda i: (0, 0, 0)),
        ],
        out_specs=(pl.BlockSpec((blk, cap, model), lambda i: (i, 0, 0)),
                   pl.BlockSpec((groups - 1, blk * cap, width), lambda i: (0, i, 0))),
        scratch_shapes=[pltpu.VMEM((blk * cap, width), jnp.bfloat16)],
        compiler_params=params(),
        cost_estimate=cost(2 * srcs * cap * (width * (ff + groups * toks) + ff * model),
                           srcs * toks * width * 2 + (width + model) * ff * 2 + srcs * cap * (ff * 4 + model * 2 + width * 2),
                           srcs * cap * ff),
        name="expert_second",
    )(slots, x_part, acc, w_in, w_out)


def base_third(g, rest, acc, w_in, w_out, srcs, cap):
    width, ff, model, blk = rest.shape[2], w_out.shape[1], w_out.shape[2], SRC_BLOCK
    last = w_in.shape[1] // width - 1
    return pl.pallas_call(
        functools.partial(third_kernel, cap),
        out_shape=jax.ShapeDtypeStruct((srcs, cap, model), jnp.bfloat16),
        grid=(srcs // blk,),
        in_specs=[
            pl.BlockSpec((1, blk * cap, width), lambda i: (g - 1, i, 0)),
            pl.BlockSpec((1, blk * cap, ff), lambda i: (g, i, 0)),
            once((1, width, ff), lambda i: (g, last, 0)),
            once((1, ff, model), lambda i: (g, 0, 0)),
        ],
        out_specs=pl.BlockSpec((blk, cap, model), lambda i: (i, 0, 0)),
        compiler_params=params(),
        cost_estimate=cost(2 * srcs * cap * (width * ff + ff * model),
                           (width + model) * ff * 2 + srcs * cap * (ff * 4 + model * 2 + width * 2), srcs * cap * ff),
        name="expert_third",
    )(rest, acc, w_in, w_out)


def over_rows(sel, slots, x_first, x_second, w_in, w_out, cap):
    srcs, toks = slots.shape
    wa, wb, ff, model, blk = x_first.shape[2], x_second.shape[2], w_out.shape[1], w_out.shape[2], OVER_BLOCK
    return pl.pallas_call(
        functools.partial(over_kernel, cap),
        out_shape=jax.ShapeDtypeStruct((srcs, cap, model), jnp.bfloat16),
        grid_spec=pltpu.PrefetchScalarGridSpec(
            num_scalar_prefetch=1,
            grid=(srcs // blk,),
            in_specs=[
                pl.BlockSpec((1, blk, toks), lambda i, sel: (i, 0, 0)),
                pl.BlockSpec((blk, toks, wa), lambda i, sel: (i, 0, 0)),
                pl.BlockSpec((blk, toks, wb), lambda i, sel: (i, 0, 0)),
                once((1, model, ff), lambda i, sel: (sel[0], 0, 0)),
                once((1, ff, model), lambda i, sel: (sel[0], 0, 0)),
            ],
            out_specs=pl.BlockSpec((blk, cap, model), lambda i, sel: (i, 0, 0)),
            scratch_shapes=[pltpu.VMEM((blk * cap, model), jnp.bfloat16)],
        ),
        compiler_params=params(),
        cost_estimate=cost(2 * srcs * cap * model * (toks + 2 * ff),
                           srcs * toks * model * 2 + 4 * ff * model + srcs * cap * model * 2, srcs * cap * ff),
        name="expert_over",
    )(sel, slots.reshape(srcs // blk, blk, toks), x_first, x_second, w_in, w_out)


def scatter_kernel(owner, axis, size, rows_ref, out_ref, local_sem, send_sem, recv_sem):
    me = lax.axis_index(axis)
    barrier = pltpu.get_barrier_semaphore()

    def send_to(k):
        dst = lax.rem(owner + k, size)
        return pltpu.make_async_remote_copy(
            src_ref=rows_ref.at[dst], dst_ref=out_ref, send_sem=send_sem.at[k], recv_sem=recv_sem,
            device_id={axis: dst}, device_id_type=pl.DeviceIdType.MESH)

    @pl.when(me != owner)
    def _():
        pl.semaphore_signal(barrier, inc=1, device_id={axis: owner}, device_id_type=pl.DeviceIdType.MESH)
        send_to(0).wait_recv()

    @pl.when(me == owner)
    def _():
        own = pltpu.make_async_copy(rows_ref.at[owner], out_ref, local_sem)
        own.start()
        pl.semaphore_wait(barrier, size - 1)
        lax.fori_loop(1, size, lambda k, c: (send_to(k).start(), c)[1], 0)
        lax.fori_loop(1, size, lambda k, c: (send_to(k).wait_send(), c)[1], 0)
        own.wait()


def scatter_from(owner, axis, size, ident, rows):
    return pl.pallas_call(
        functools.partial(scatter_kernel, owner, axis, size),
        out_shape=jax.ShapeDtypeStruct(rows.shape[1:], rows.dtype),
        in_specs=[pl.BlockSpec(memory_space=pl.ANY)],
        out_specs=pl.BlockSpec(memory_space=pl.ANY),
        scratch_shapes=[pltpu.SemaphoreType.DMA, pltpu.SemaphoreType.DMA((size,)), pltpu.SemaphoreType.DMA],
        compiler_params=pltpu.CompilerParams(collective_id=ident, has_side_effects=True),
        name="scatter_over",
    )(rows)


def solution(mesh):
    group_size = mesh.shape['ep']

    def local_layer(x_loc, idx_loc, gate_loc, w_in, w_out, shared_in, shared_out):
        tok_rows, top_k = idx_loc.shape
        model = x_loc.shape[1]
        own = w_in.shape[0]
        num_experts = own * group_size
        slot_cap = min(tok_rows, LOAD_MULT * tok_rows * top_k // num_experts)
        cap = BASE_CAP
        over_cap = slot_cap - cap
        cut = model * 3 // 4
        me = lax.axis_index('ep')
        experts = jnp.arange(num_experts, dtype=jnp.int32)

        before = (lax.broadcasted_iota(jnp.int32, (tok_rows, tok_rows), 0)
                  <= lax.broadcasted_iota(jnp.int32, (tok_rows, tok_rows), 1)).astype(jnp.bfloat16)

        def slots_of(hit):
            count = jnp.dot(hit.reshape(-1, tok_rows).astype(jnp.bfloat16), before, preferred_element_type=jnp.float32)
            return jnp.where(hit, count.reshape(hit.shape).astype(jnp.int32) - 1, -1)

        def gather_with(part, extra):
            extra = jnp.pad(extra.astype(jnp.bfloat16), ((0, EXTRA_ROWS - extra.shape[0]), (0, part.shape[1] - extra.shape[1])))
            return lax.all_gather(jnp.concatenate([part, extra], axis=0), 'ep')

        idx_t = idx_loc.T
        x_first = gather_with(x_loc[:, :cut], idx_t)

        gate_t = gate_loc.astype(jnp.bfloat16).T
        same = idx_t[None] == experts[:, None, None]
        hit_loc = jnp.any(same, axis=1)
        gate_of = jnp.sum(jnp.where(same, gate_t[None], 0).astype(jnp.float32), axis=1).astype(jnp.bfloat16)
        slot_loc = slots_of(hit_loc)
        count_loc = jnp.max(slot_loc, axis=1) + 1

        x_second = gather_with(x_loc[:, cut:], count_loc[None])

        def combine_table(g):
            slot = slot_loc.reshape(group_size, own, 1, tok_rows)[:, g]
            gate = gate_of.reshape(group_size, own, 1, tok_rows)[:, g]
            pick = slot == jnp.arange(cap, dtype=jnp.int32)[None, :, None]
            return jnp.where(pick, gate, 0).astype(jnp.bfloat16).reshape(group_size * cap, tok_rows)

        def weigh(comb, rows):
            return lax.dot_general(comb, rows, (((0,), (0,)), ((), ())), preferred_element_type=jnp.float32)

        shared_hidden = gelu(jnp.dot(x_loc, shared_in, preferred_element_type=jnp.float32)).astype(jnp.bfloat16)
        shared_val = jnp.dot(shared_hidden, shared_out, preferred_element_type=jnp.float32)
        combs = [combine_table(g) for g in range(own)]
        x_first, shared_val, combs = lax.optimization_barrier((x_first, shared_val, combs))

        idx_all = x_first[:, tok_rows:tok_rows + top_k, :tok_rows].astype(jnp.int32)

        def slots_all(expert):
            return slots_of(jnp.any(idx_all == expert, axis=1))

        base_slots = jnp.stack([slots_all(me * own + g) for g in range(own)])
        acc = base_first(base_slots, x_first, w_in, cap)
        x_second, acc = lax.optimization_barrier((x_second, acc))
        out, rest = base_second(base_slots, x_second, acc, w_in, w_out, cap)
        outs = [out]
        for g in range(1, own):
            outs.append(base_third(g, rest, acc, w_in, w_out, group_size, cap))
        backs = [lax.all_to_all(out, 'ep', 0, 0, tiled=True) for out in outs]

        x_over, x_over_b, _ = lax.optimization_barrier((x_first, x_second, outs[-1]))
        load = jnp.max(x_over_b[:, tok_rows, :num_experts].astype(jnp.int32), axis=0)
        over = load > cap
        over_rank = jnp.sum((over[None, :] & (experts[None, :] < experts[:, None])).astype(jnp.int32), axis=1)
        num_over = jnp.sum(over.astype(jnp.int32))

        def over_expert(i):
            chosen = over & (over_rank == i)
            return jnp.where(i < num_over, jnp.sum(jnp.where(chosen, experts, 0)), num_experts)

        def over_compute(expert):
            mine = expert // own == me
            sel = jnp.where(mine, expert % own, 0).reshape(1)
            return lax.cond(
                mine, lambda: over_rows(sel, slots_all(expert) - cap, x_over, x_over_b, w_in, w_out, over_cap),
                lambda: jnp.zeros((group_size, over_cap, model), jnp.bfloat16))

        def over_combine(expert, rows):
            at = jnp.minimum(expert, num_experts - 1)
            slot = lax.dynamic_index_in_dim(slot_loc, at, 0, keepdims=True)
            gate = lax.dynamic_index_in_dim(gate_of, at, 0, keepdims=True)
            pick = (slot - cap == lax.broadcasted_iota(jnp.int32, (over_cap, tok_rows), 0)) & (expert < num_experts)
            return weigh(jnp.where(pick, gate, 0).astype(jnp.bfloat16), rows)

        total = shared_val
        over_ids = [over_expert(i) for i in range(HOT_STATIC)]
        over_outs = lax.optimization_barrier([over_compute(expert) for expert in over_ids])
        for i, (expert, rows) in enumerate(zip(over_ids, over_outs)):
            owner = jnp.minimum(expert, num_experts - 1) // own
            mine = lax.switch(owner, [functools.partial(scatter_from, d, 'ep', group_size, i) for d in range(group_size)], rows)
            total = total + over_combine(expert, mine)

        def more(i, total):
            expert = over_expert(i)
            rows = over_compute(expert).reshape(group_size * over_cap, model)
            rows = lax.psum_scatter(rows, 'ep', scatter_dimension=0, tiled=True)
            return total + over_combine(expert, rows)

        total = lax.fori_loop(HOT_STATIC, jnp.maximum(num_over, HOT_STATIC), more, total)
        for comb, back in zip(combs[:-1], backs[:-1]):
            total = total + weigh(comb, back.reshape(group_size * cap, model))
        total, back = lax.optimization_barrier((total, backs[-1]))
        return (total + weigh(combs[-1], back.reshape(group_size * cap, model))).astype(jnp.bfloat16)

    tok_spec = P(('dp', 'ep'), None)
    expert_spec = P('ep', None, None)
    whole_spec = P(None, None)
    return jax.shard_map(local_layer, mesh=mesh, in_specs=(tok_spec, tok_spec, tok_spec, expert_spec, expert_spec, whole_spec, whole_spec), out_specs=tok_spec, check_vma=False)
```

```python
import functools
import math

import jax
import jax.numpy as jnp
from jax import lax
from jax.experimental import pallas as pl
from jax.experimental.pallas import tpu as pltpu
from jax.sharding import PartitionSpec as P

LOAD_MULT = 3
BASE_CAP = 48
HOT_STATIC = 2
SRC_BLOCK = 8
COMBINE_BLOCK = 512
EXTRA_ROWS = 16
VMEM = 60 * 2 ** 20


def gelu(z):
    return jax.nn.gelu(z, approximate=True)


def gather_rows(slot_ref, x_ref, cap, put):
    groups, blk, toks = slot_ref.shape
    slot_iota = lax.broadcasted_iota(jnp.int32, (cap, toks), 0)

    def one(s, carry):
        picks = [(slot_iota == slot_ref[g, pl.ds(s, 1), :]).astype(jnp.bfloat16) for g in range(groups)]
        pick = jnp.concatenate(picks, axis=0) if groups > 1 else picks[0]
        got = jnp.dot(pick, x_ref[s], preferred_element_type=jnp.float32).astype(jnp.bfloat16)
        for g in range(groups):
            put(g, pl.ds(pl.multiple_of(s * cap, 16), cap), got[g * cap:(g + 1) * cap])
        return carry

    lax.fori_loop(0, blk, one, 0)


def first_kernel(cap, sel_ref, slot_ref, x_ref, w_ref, acc_ref, rows_ref):
    def put(g, where, rows):
        rows_ref[g, where, :] = rows

    gather_rows(slot_ref, x_ref, cap, put)
    for g in range(w_ref.shape[0]):
        acc_ref[g] = jnp.dot(rows_ref[g], w_ref[g], preferred_element_type=jnp.float32)


def second_kernel(cap, sel_ref, slot_ref, x_ref, acc_ref, w_ref, v_ref, out_ref, rows_ref):
    def put(g, where, rows):
        rows_ref[g, where, :] = rows

    gather_rows(slot_ref, x_ref, cap, put)
    for g in range(w_ref.shape[0]):
        pre = acc_ref[g] + jnp.dot(rows_ref[g], w_ref[g], preferred_element_type=jnp.float32)
        hid = gelu(pre).astype(jnp.bfloat16)
        out = jnp.dot(hid, v_ref[g], preferred_element_type=jnp.float32).astype(jnp.bfloat16)
        out_ref[:, g * cap:(g + 1) * cap] = out.reshape(out_ref.shape[0], cap, out_ref.shape[2])


def combine_kernel(comb_ref, back_ref, part_ref, out_ref):
    routed = jnp.dot(comb_ref[...], back_ref[...], preferred_element_type=jnp.float32)
    out_ref[...] = (part_ref[...] + routed).astype(out_ref.dtype)


def params():
    return pltpu.CompilerParams(dimension_semantics=("arbitrary",), vmem_limit_bytes=VMEM)


def cost(flops, nbytes, trans=0):
    return pl.CostEstimate(flops=int(flops), bytes_accessed=int(nbytes), transcendentals=int(trans))


def once(shape, index):
    return pl.BlockSpec(shape, index, pipeline_mode=pl.Buffered(1))


def expert_first(sel, slots, x_part, w_in, cap):
    groups, srcs, toks = slots.shape
    width, ff, blk = x_part.shape[2], w_in.shape[2], SRC_BLOCK
    return pl.pallas_call(
        functools.partial(first_kernel, cap),
        out_shape=jax.ShapeDtypeStruct((groups, srcs * cap, ff), jnp.float32),
        grid_spec=pltpu.PrefetchScalarGridSpec(
            num_scalar_prefetch=1,
            grid=(srcs // blk,),
            in_specs=[
                pl.BlockSpec((groups, blk, toks), lambda i, sel: (0, i, 0)),
                pl.BlockSpec((blk, toks, width), lambda i, sel: (i, 0, 0)),
                once((groups, width, ff), lambda i, sel: (sel[0], 0, 0)),
            ],
            out_specs=pl.BlockSpec((groups, blk * cap, ff), lambda i, sel: (0, i, 0)),
            scratch_shapes=[pltpu.VMEM((groups, blk * cap, width), jnp.bfloat16)],
        ),
        compiler_params=params(),
        cost_estimate=cost(2 * groups * srcs * cap * width * (ff + toks),
                           srcs * toks * width * 2 + groups * (width * ff * 2 + srcs * cap * ff * 4)),
        name="expert_first",
    )(sel, slots, x_part, w_in)


def expert_second(sel, slots, x_part, acc, w_in, w_out, cap):
    groups, srcs, toks = slots.shape
    width, ff, model, blk = x_part.shape[2], w_out.shape[1], w_out.shape[2], SRC_BLOCK
    last = w_in.shape[1] // width - 1
    return pl.pallas_call(
        functools.partial(second_kernel, cap),
        out_shape=jax.ShapeDtypeStruct((srcs, groups * cap, model), jnp.bfloat16),
        grid_spec=pltpu.PrefetchScalarGridSpec(
            num_scalar_prefetch=1,
            grid=(srcs // blk,),
            in_specs=[
                pl.BlockSpec((groups, blk, toks), lambda i, sel: (0, i, 0)),
                pl.BlockSpec((blk, toks, width), lambda i, sel: (i, 0, 0)),
                pl.BlockSpec((groups, blk * cap, ff), lambda i, sel: (0, i, 0)),
                once((groups, width, ff), lambda i, sel: (sel[0], last, 0)),
                once((groups, ff, model), lambda i, sel: (sel[0], 0, 0)),
            ],
            out_specs=pl.BlockSpec((blk, groups * cap, model), lambda i, sel: (i, 0, 0)),
            scratch_shapes=[pltpu.VMEM((groups, blk * cap, width), jnp.bfloat16)],
        ),
        compiler_params=params(),
        cost_estimate=cost(2 * groups * srcs * cap * (width * (ff + toks) + ff * model),
                           srcs * toks * width * 2 + groups * ((width + model) * ff * 2 + srcs * cap * (ff * 4 + model * 2)),
                           groups * srcs * cap * ff),
        name="expert_second",
    )(sel, slots, x_part, acc, w_in, w_out)


def combine(comb, back, part):
    toks, pairs = comb.shape
    model, blk = back.shape[1], COMBINE_BLOCK
    return pl.pallas_call(
        combine_kernel,
        out_shape=jax.ShapeDtypeStruct((toks, model), jnp.bfloat16),
        grid=(model // blk,),
        in_specs=[
            once((toks, pairs), lambda i: (0, 0)),
            pl.BlockSpec((pairs, blk), lambda i: (0, i)),
            pl.BlockSpec((toks, blk), lambda i: (0, i)),
        ],
        out_specs=pl.BlockSpec((toks, blk), lambda i: (0, i)),
        compiler_params=params(),
        cost_estimate=cost(2 * toks * pairs * model, pairs * (toks + model) * 2 + toks * model * 6),
        name="combine",
    )(comb, back, part)


def scatter_kernel(owner, axis, size, rows_ref, out_ref, local_sem, send_sem, recv_sem):
    me = lax.axis_index(axis)
    barrier = pltpu.get_barrier_semaphore()
    stride = next(n for n in range(size // 3 | 1, 2 * size) if math.gcd(n, size) == 1)

    def send_to(k):
        dst = lax.rem(owner + k * stride, size)
        return pltpu.make_async_remote_copy(
            src_ref=rows_ref.at[dst], dst_ref=out_ref, send_sem=send_sem.at[k], recv_sem=recv_sem,
            device_id={axis: dst}, device_id_type=pl.DeviceIdType.MESH)

    @pl.when(me != owner)
    def _():
        pl.semaphore_signal(barrier, inc=1, device_id={axis: owner}, device_id_type=pl.DeviceIdType.MESH)
        send_to(0).wait_recv()

    @pl.when(me == owner)
    def _():
        own = pltpu.make_async_copy(rows_ref.at[owner], out_ref, local_sem)
        own.start()
        pl.semaphore_wait(barrier, size - 1)
        lax.fori_loop(1, size, lambda k, c: (send_to(k).start(), c)[1], 0)
        lax.fori_loop(1, size, lambda k, c: (send_to(k).wait_send(), c)[1], 0)
        own.wait()


def scatter_from(owner, axis, size, ident, rows):
    return pl.pallas_call(
        functools.partial(scatter_kernel, owner, axis, size),
        out_shape=jax.ShapeDtypeStruct(rows.shape[1:], rows.dtype),
        in_specs=[pl.BlockSpec(memory_space=pl.ANY)],
        out_specs=pl.BlockSpec(memory_space=pl.ANY),
        scratch_shapes=[pltpu.SemaphoreType.DMA, pltpu.SemaphoreType.DMA((size,)), pltpu.SemaphoreType.DMA],
        compiler_params=pltpu.CompilerParams(collective_id=ident, has_side_effects=True),
        name="scatter_over",
    )(rows)


def solution(mesh):
    group_size = mesh.shape['ep']

    def local_layer(x_loc, idx_loc, gate_loc, w_in, w_out, shared_in, shared_out):
        tok_rows, top_k = idx_loc.shape
        model = x_loc.shape[1]
        own = w_in.shape[0]
        num_experts = own * group_size
        slot_cap = min(tok_rows, LOAD_MULT * tok_rows * top_k // num_experts)
        cap = BASE_CAP
        over_cap = slot_cap - cap
        cut = model * 3 // 4
        me = lax.axis_index('ep')
        experts = jnp.arange(num_experts, dtype=jnp.int32)

        before = (lax.broadcasted_iota(jnp.int32, (tok_rows, tok_rows), 0)
                  <= lax.broadcasted_iota(jnp.int32, (tok_rows, tok_rows), 1)).astype(jnp.bfloat16)

        def slots_of(hit):
            count = jnp.dot(hit.reshape(-1, tok_rows).astype(jnp.bfloat16), before, preferred_element_type=jnp.float32)
            return jnp.where(hit, count.reshape(hit.shape).astype(jnp.int32) - 1, -1)

        idx_t = idx_loc.T
        count_loc = jnp.sum((idx_t.reshape(1, -1) == experts[:, None]).astype(jnp.int32), axis=1)
        meta = jnp.concatenate([idx_t, jnp.pad(count_loc[None], ((0, 0), (0, tok_rows - num_experts)))], axis=0)
        meta = jnp.pad(meta.astype(jnp.bfloat16), ((0, EXTRA_ROWS - top_k - 1), (0, cut - tok_rows)))
        x_first = lax.all_gather(jnp.concatenate([x_loc[:, :cut], meta], axis=0), 'ep')
        x_second = lax.all_gather(x_loc[:, cut:], 'ep')

        gate_t = gate_loc.astype(jnp.bfloat16).T
        same = idx_t[None] == experts[:, None, None]
        hit_loc = jnp.any(same, axis=1)
        gate_of = jnp.sum(jnp.where(same, gate_t[None], 0).astype(jnp.float32), axis=1).astype(jnp.bfloat16)
        slot_loc = slots_of(hit_loc)

        pick = slot_loc[:, None, :] == jnp.arange(cap, dtype=jnp.int32)[None, :, None]
        comb = jnp.where(pick, gate_of[:, None, :], 0).astype(jnp.bfloat16).reshape(num_experts * cap, tok_rows).T

        def weigh(comb, rows):
            return lax.dot_general(comb, rows, (((0,), (0,)), ((), ())), preferred_element_type=jnp.float32)

        shared_hidden = gelu(jnp.dot(x_loc, shared_in, preferred_element_type=jnp.float32)).astype(jnp.bfloat16)
        shared_val = jnp.dot(shared_hidden, shared_out, preferred_element_type=jnp.float32)
        x_first, shared_val, comb = lax.optimization_barrier((x_first, shared_val, comb))

        idx_all = x_first[:, tok_rows:tok_rows + top_k, :tok_rows].astype(jnp.int32)
        load = jnp.max(x_first[:, tok_rows + top_k, :num_experts].astype(jnp.int32), axis=0)

        def slots_all(expert):
            return slots_of(jnp.any(idx_all == expert, axis=1))

        over = load > cap
        over_rank = jnp.sum((over[None, :] & (experts[None, :] < experts[:, None])).astype(jnp.int32), axis=1)
        num_over = jnp.sum(over.astype(jnp.int32))

        def over_expert(i):
            chosen = over & (over_rank == i)
            return jnp.where(i < num_over, jnp.sum(jnp.where(chosen, experts, 0)), num_experts)

        def over_setup(i):
            expert = over_expert(i)
            mine = expert // own == me
            return expert, mine, jnp.where(mine, expert % own, 0).reshape(1), (slots_all(expert) - cap)[None]

        def over_first(setup, x_part):
            expert, mine, sel, slots = setup
            return lax.cond(
                mine, lambda: expert_first(sel, slots, x_part, w_in, over_cap),
                lambda: jnp.zeros((1, group_size * over_cap, w_in.shape[2]), jnp.float32))

        def over_second(setup, x_part, acc):
            expert, mine, sel, slots = setup
            return lax.cond(
                mine, lambda: expert_second(sel, slots, x_part, acc, w_in, w_out, over_cap),
                lambda: jnp.zeros((group_size, over_cap, model), jnp.bfloat16))

        base_sel = jnp.zeros((1,), jnp.int32)
        base_slots = jnp.stack([slots_all(me * own + g) for g in range(own)])
        acc = expert_first(base_sel, base_slots, x_first, w_in, cap)
        setups = [over_setup(i) for i in range(HOT_STATIC)]
        over_accs = [over_first(setup, x_first) for setup in setups]
        x_second, acc, over_accs = lax.optimization_barrier((x_second, acc, over_accs))
        out = expert_second(base_sel, base_slots, x_second, acc, w_in, w_out, cap)
        back = lax.all_to_all(out, 'ep', 0, 0, tiled=True).reshape(num_experts * cap, model)
        x_over, over_accs, _ = lax.optimization_barrier((x_second, over_accs, out))
        over_outs = lax.optimization_barrier([over_second(s, x_over, a) for s, a in zip(setups, over_accs)])

        def over_combine(expert, rows):
            at = jnp.minimum(expert, num_experts - 1)
            slot = lax.dynamic_index_in_dim(slot_loc, at, 0, keepdims=True)
            gate = lax.dynamic_index_in_dim(gate_of, at, 0, keepdims=True)
            pick = (slot - cap == lax.broadcasted_iota(jnp.int32, (over_cap, tok_rows), 0)) & (expert < num_experts)
            return weigh(jnp.where(pick, gate, 0).astype(jnp.bfloat16), rows)

        total = shared_val
        for i, (setup, rows) in enumerate(zip(setups, over_outs)):
            expert = setup[0]
            owner = jnp.minimum(expert, num_experts - 1) // own
            mine = lax.switch(owner, [functools.partial(scatter_from, d, 'ep', group_size, i) for d in range(group_size)], rows)
            total = total + over_combine(expert, mine)

        def more(i, total):
            setup = over_setup(i)
            rows = over_second(setup, x_over, over_first(setup, x_first)).reshape(group_size * over_cap, model)
            rows = lax.psum_scatter(rows, 'ep', scatter_dimension=0, tiled=True)
            return total + over_combine(setup[0], rows)

        total = lax.fori_loop(HOT_STATIC, jnp.maximum(num_over, HOT_STATIC), more, total)
        return combine(comb, back, total)

    tok_spec = P(('dp', 'ep'), None)
    expert_spec = P('ep', None, None)
    whole_spec = P(None, None)
    return jax.shard_map(local_layer, mesh=mesh, in_specs=(tok_spec, tok_spec, tok_spec, expert_spec, expert_spec, whole_spec, whole_spec), out_specs=tok_spec, check_vma=False)
```

```python
import functools
import math

import jax
import jax.numpy as jnp
from jax import lax
from jax.experimental import pallas as pl
from jax.experimental.pallas import tpu as pltpu
from jax.sharding import PartitionSpec as P


LOAD_MULT = 3
BASE_CAP = 48
HOT_STATIC = 2
SRC_BLOCK = 8
COMBINE_BLOCK = 512
EXTRA_ROWS = 16
VMEM = 60 * 2 ** 20


def gelu(z):
    return jax.nn.gelu(z, approximate=True)


def gather_rows(slot_ref, x_ref, cap, put):
    groups, blk, toks = slot_ref.shape
    slot_iota = lax.broadcasted_iota(jnp.int32, (cap, toks), 0)

    def one(s, carry):
        picks = [(slot_iota == slot_ref[g, pl.ds(s, 1), :]).astype(jnp.bfloat16) for g in range(groups)]
        pick = jnp.concatenate(picks, axis=0) if groups > 1 else picks[0]
        got = jnp.dot(pick, x_ref[s], preferred_element_type=jnp.float32).astype(jnp.bfloat16)
        for g in range(groups):
            put(g, pl.ds(pl.multiple_of(s * cap, 16), cap), got[g * cap:(g + 1) * cap])
        return carry

    lax.fori_loop(0, blk, one, 0)


def first_kernel(cap, sel_ref, slot_ref, x_ref, w_ref, acc_ref, rows_ref):
    def put(g, where, rows):
        rows_ref[g, where, :] = rows

    gather_rows(slot_ref, x_ref, cap, put)
    for g in range(w_ref.shape[0]):
        acc_ref[g] = jnp.dot(rows_ref[g], w_ref[g], preferred_element_type=jnp.float32)


def second_kernel(cap, sel_ref, slot_ref, x_ref, acc_ref, w_ref, v_ref, out_ref, rows_ref):
    def put(g, where, rows):
        rows_ref[g, where, :] = rows

    gather_rows(slot_ref, x_ref, cap, put)
    for g in range(w_ref.shape[0]):
        pre = acc_ref[g] + jnp.dot(rows_ref[g], w_ref[g], preferred_element_type=jnp.float32)
        hid = gelu(pre).astype(jnp.bfloat16)
        out = jnp.dot(hid, v_ref[g], preferred_element_type=jnp.float32).astype(jnp.bfloat16)
        out_ref[:, g * cap:(g + 1) * cap] = out.reshape(out_ref.shape[0], cap, out_ref.shape[2])


def combine_kernel(comb_ref, back_ref, part_ref, out_ref):
    routed = jnp.dot(comb_ref[...], back_ref[...], preferred_element_type=jnp.float32)
    out_ref[...] = (part_ref[...] + routed).astype(out_ref.dtype)


def params():
    return pltpu.CompilerParams(dimension_semantics=("arbitrary",), vmem_limit_bytes=VMEM)


def cost(flops, nbytes, trans=0):
    return pl.CostEstimate(flops=int(flops), bytes_accessed=int(nbytes), transcendentals=int(trans))


def once(shape, index):
    return pl.BlockSpec(shape, index, pipeline_mode=pl.Buffered(1))


def expert_first(sel, slots, x_part, w_in, cap):
    groups, srcs, toks = slots.shape
    width, ff, blk = x_part.shape[2], w_in.shape[2], SRC_BLOCK
    return pl.pallas_call(
        functools.partial(first_kernel, cap),
        out_shape=jax.ShapeDtypeStruct((groups, srcs * cap, ff), jnp.float32),
        grid_spec=pltpu.PrefetchScalarGridSpec(
            num_scalar_prefetch=1,
            grid=(srcs // blk,),
            in_specs=[
                pl.BlockSpec((groups, blk, toks), lambda i, sel: (0, i, 0)),
                pl.BlockSpec((blk, toks, width), lambda i, sel: (i, 0, 0)),
                once((groups, width, ff), lambda i, sel: (sel[0], 0, 0)),
            ],
            out_specs=pl.BlockSpec((groups, blk * cap, ff), lambda i, sel: (0, i, 0)),
            scratch_shapes=[pltpu.VMEM((groups, blk * cap, width), jnp.bfloat16)],
        ),
        compiler_params=params(),
        cost_estimate=cost(2 * groups * srcs * cap * width * (ff + toks),
                           srcs * toks * width * 2 + groups * (width * ff * 2 + srcs * cap * ff * 4)),
        name="expert_first",
    )(sel, slots, x_part, w_in)


def expert_second(sel, slots, x_part, acc, w_in, w_out, cap):
    groups, srcs, toks = slots.shape
    width, ff, model, blk = x_part.shape[2], w_out.shape[1], w_out.shape[2], SRC_BLOCK
    last = w_in.shape[1] // width - 1
    return pl.pallas_call(
        functools.partial(second_kernel, cap),
        out_shape=jax.ShapeDtypeStruct((srcs, groups * cap, model), jnp.bfloat16),
        grid_spec=pltpu.PrefetchScalarGridSpec(
            num_scalar_prefetch=1,
            grid=(srcs // blk,),
            in_specs=[
                pl.BlockSpec((groups, blk, toks), lambda i, sel: (0, i, 0)),
                pl.BlockSpec((blk, toks, width), lambda i, sel: (i, 0, 0)),
                pl.BlockSpec((groups, blk * cap, ff), lambda i, sel: (0, i, 0)),
                once((groups, width, ff), lambda i, sel: (sel[0], last, 0)),
                once((groups, ff, model), lambda i, sel: (sel[0], 0, 0)),
            ],
            out_specs=pl.BlockSpec((blk, groups * cap, model), lambda i, sel: (i, 0, 0)),
            scratch_shapes=[pltpu.VMEM((groups, blk * cap, width), jnp.bfloat16)],
        ),
        compiler_params=params(),
        cost_estimate=cost(2 * groups * srcs * cap * (width * (ff + toks) + ff * model),
                           srcs * toks * width * 2 + groups * ((width + model) * ff * 2 + srcs * cap * (ff * 4 + model * 2)),
                           groups * srcs * cap * ff),
        name="expert_second",
    )(sel, slots, x_part, acc, w_in, w_out)


def combine(comb, back, part):
    toks, pairs = comb.shape
    model, blk = back.shape[1], COMBINE_BLOCK
    return pl.pallas_call(
        combine_kernel,
        out_shape=jax.ShapeDtypeStruct((toks, model), jnp.bfloat16),
        grid=(model // blk,),
        in_specs=[
            once((toks, pairs), lambda i: (0, 0)),
            pl.BlockSpec((pairs, blk), lambda i: (0, i)),
            pl.BlockSpec((toks, blk), lambda i: (0, i)),
        ],
        out_specs=pl.BlockSpec((toks, blk), lambda i: (0, i)),
        compiler_params=params(),
        cost_estimate=cost(2 * toks * pairs * model, pairs * (toks + model) * 2 + toks * model * 6),
        name="combine",
    )(comb, back, part)


def scatter_kernel(owner, axis, size, rows_ref, out_ref, local_sem, send_sem, recv_sem):
    me = lax.axis_index(axis)
    barrier = pltpu.get_barrier_semaphore()
    stride = next(n for n in range(size // 3 | 1, 2 * size) if math.gcd(n, size) == 1)

    def send_to(k):
        dst = lax.rem(owner + k * stride, size)
        return pltpu.make_async_remote_copy(
            src_ref=rows_ref.at[dst], dst_ref=out_ref, send_sem=send_sem.at[k], recv_sem=recv_sem,
            device_id={axis: dst}, device_id_type=pl.DeviceIdType.MESH)

    @pl.when(me != owner)
    def _():
        pl.semaphore_signal(barrier, inc=1, device_id={axis: owner}, device_id_type=pl.DeviceIdType.MESH)
        send_to(0).wait_recv()

    @pl.when(me == owner)
    def _():
        own = pltpu.make_async_copy(rows_ref.at[owner], out_ref, local_sem)
        own.start()
        pl.semaphore_wait(barrier, size - 1)
        lax.fori_loop(1, size, lambda k, c: (send_to(k).start(), c)[1], 0)
        lax.fori_loop(1, size, lambda k, c: (send_to(k).wait_send(), c)[1], 0)
        own.wait()


def scatter_from(owner, axis, size, ident, rows):
    return pl.pallas_call(
        functools.partial(scatter_kernel, owner, axis, size),
        out_shape=jax.ShapeDtypeStruct(rows.shape[1:], rows.dtype),
        in_specs=[pl.BlockSpec(memory_space=pltpu.VMEM)],
        out_specs=pl.BlockSpec(memory_space=pl.ANY),
        scratch_shapes=[pltpu.SemaphoreType.DMA, pltpu.SemaphoreType.DMA((size,)), pltpu.SemaphoreType.DMA],
        compiler_params=pltpu.CompilerParams(collective_id=ident, has_side_effects=True, vmem_limit_bytes=32 * 2 ** 20),
        name="scatter_over",
    )(rows)


def solution(mesh):
    group_size = mesh.shape['ep']

    def local_layer(x_loc, idx_loc, gate_loc, w_in, w_out, shared_in, shared_out):
        tok_rows, top_k = idx_loc.shape
        model = x_loc.shape[1]
        own = w_in.shape[0]
        num_experts = own * group_size
        slot_cap = min(tok_rows, LOAD_MULT * tok_rows * top_k // num_experts)
        cap = BASE_CAP
        over_cap = slot_cap - cap
        cut = model * 3 // 4
        me = lax.axis_index('ep')
        experts = jnp.arange(num_experts, dtype=jnp.int32)

        before = (lax.broadcasted_iota(jnp.int32, (tok_rows, tok_rows), 0)
                  <= lax.broadcasted_iota(jnp.int32, (tok_rows, tok_rows), 1)).astype(jnp.bfloat16)

        def slots_of(hit):
            count = jnp.dot(hit.reshape(-1, tok_rows).astype(jnp.bfloat16), before, preferred_element_type=jnp.float32)
            return jnp.where(hit, count.reshape(hit.shape).astype(jnp.int32) - 1, -1)

        idx_t = idx_loc.T
        count_loc = jnp.sum((idx_t.reshape(1, -1) == experts[:, None]).astype(jnp.int32), axis=1)
        meta = jnp.concatenate([idx_t, jnp.pad(count_loc[None], ((0, 0), (0, tok_rows - num_experts)))], axis=0)
        meta = jnp.pad(meta.astype(jnp.bfloat16), ((0, EXTRA_ROWS - top_k - 1), (0, cut - tok_rows)))
        x_first = lax.all_gather(jnp.concatenate([x_loc[:, :cut], meta], axis=0), 'ep')
        x_second = lax.all_gather(x_loc[:, cut:], 'ep')

        gate_t = gate_loc.astype(jnp.bfloat16).T
        same = idx_t[None] == experts[:, None, None]
        hit_loc = jnp.any(same, axis=1)
        gate_of = jnp.sum(jnp.where(same, gate_t[None], 0).astype(jnp.float32), axis=1).astype(jnp.bfloat16)
        slot_loc = slots_of(hit_loc)

        pick = slot_loc[:, None, :] == jnp.arange(cap, dtype=jnp.int32)[None, :, None]
        comb = jnp.where(pick, gate_of[:, None, :], 0).astype(jnp.bfloat16).reshape(num_experts * cap, tok_rows).T

        def weigh(comb, rows):
            return lax.dot_general(comb, rows, (((0,), (0,)), ((), ())), preferred_element_type=jnp.float32)

        shared_hidden = gelu(jnp.dot(x_loc, shared_in, preferred_element_type=jnp.float32)).astype(jnp.bfloat16)
        shared_val = jnp.dot(shared_hidden, shared_out, preferred_element_type=jnp.float32)
        x_first, shared_val, comb = lax.optimization_barrier((x_first, shared_val, comb))

        idx_all = x_first[:, tok_rows:tok_rows + top_k, :tok_rows].astype(jnp.int32)
        load = jnp.max(x_first[:, tok_rows + top_k, :num_experts].astype(jnp.int32), axis=0)

        def slots_all(expert):
            return slots_of(jnp.any(idx_all == expert, axis=1))

        over = load > cap
        over_rank = jnp.sum((over[None, :] & (experts[None, :] < experts[:, None])).astype(jnp.int32), axis=1)
        num_over = jnp.sum(over.astype(jnp.int32))

        def over_expert(i):
            chosen = over & (over_rank == i)
            return jnp.where(i < num_over, jnp.sum(jnp.where(chosen, experts, 0)), num_experts)

        def over_setup(i):
            expert = over_expert(i)
            mine = expert // own == me
            return expert, mine, jnp.where(mine, expert % own, 0).reshape(1), (slots_all(expert) - cap)[None]

        def over_first(setup, x_part):
            _, mine, sel, slots = setup
            return lax.cond(
                mine, lambda: expert_first(sel, slots, x_part, w_in, over_cap),
                lambda: jnp.zeros((1, group_size * over_cap, w_in.shape[2]), jnp.float32))

        def over_second(setup, x_part, acc):
            _, mine, sel, slots = setup
            return lax.cond(
                mine, lambda: expert_second(sel, slots, x_part, acc, w_in, w_out, over_cap),
                lambda: jnp.zeros((group_size, over_cap, model), jnp.bfloat16))

        base_sel = jnp.zeros((1,), jnp.int32)
        base_slots = jnp.stack([slots_all(me * own + g) for g in range(own)])
        acc = expert_first(base_sel, base_slots, x_first, w_in, cap)
        setups = [over_setup(i) for i in range(HOT_STATIC)]
        over_accs = [over_first(setup, x_first) for setup in setups]
        x_second, acc, over_accs = lax.optimization_barrier((x_second, acc, over_accs))
        out = expert_second(base_sel, base_slots, x_second, acc, w_in, w_out, cap)
        back = lax.all_to_all(out, 'ep', 0, 0, tiled=True).reshape(num_experts * cap, model)
        x_over, over_accs, _ = lax.optimization_barrier((x_second, over_accs, out))
        over_outs = [over_second(s, x_over, a) for s, a in zip(setups, over_accs)]
        over_outs = lax.optimization_barrier(over_outs)

        def over_combine(expert, rows):
            at = jnp.minimum(expert, num_experts - 1)
            slot = lax.dynamic_index_in_dim(slot_loc, at, 0, keepdims=True)
            gate = lax.dynamic_index_in_dim(gate_of, at, 0, keepdims=True)
            pick = (slot - cap == lax.broadcasted_iota(jnp.int32, (over_cap, tok_rows), 0)) & (expert < num_experts)
            return weigh(jnp.where(pick, gate, 0).astype(jnp.bfloat16), rows)

        def scatter(setup, rows):
            owner = jnp.minimum(setup[0], num_experts - 1) // own
            return lax.switch(owner, [functools.partial(scatter_from, d, 'ep', group_size, 0) for d in range(group_size)], rows)

        def spread(rows):
            return lax.psum_scatter(rows.reshape(group_size * over_cap, model), 'ep', scatter_dimension=0, tiled=True)

        rest = [spread(rows) for rows in over_outs[1:]]
        total = shared_val + over_combine(setups[0][0], scatter(setups[0], over_outs[0]))
        for setup, rows in zip(setups[1:], rest):
            total = total + over_combine(setup[0], rows)

        def more(i, total):
            setup = over_setup(i)
            return total + over_combine(setup[0], spread(over_second(setup, x_over, over_first(setup, x_first))))

        total = lax.fori_loop(HOT_STATIC, jnp.maximum(num_over, HOT_STATIC), more, total)
        return combine(comb, back, total)

    tok_spec = P(('dp', 'ep'), None)
    expert_spec = P('ep', None, None)
    whole_spec = P(None, None)
    return jax.shard_map(local_layer, mesh=mesh, in_specs=(tok_spec, tok_spec, tok_spec, expert_spec, expert_spec, whole_spec, whole_spec), out_specs=tok_spec, check_vma=False)
```

```python
import functools
import math

import jax
import jax.numpy as jnp
from jax import lax
from jax.experimental import pallas as pl
from jax.experimental.pallas import tpu as pltpu
from jax.sharding import PartitionSpec as P


LOAD_MULT = 3
BASE_CAP = 48
HOT_STATIC = 2
SRC_BLOCK = 8
COMBINE_BLOCK = 512
EXTRA_ROWS = 16
VMEM = 60 * 2 ** 20


def gelu(z):
    return jax.nn.gelu(z, approximate=True)


def gather_rows(slot_ref, x_ref, cap, put):
    groups, blk, toks = slot_ref.shape
    slot_iota = lax.broadcasted_iota(jnp.int32, (cap, toks), 0)

    def one(s, carry):
        picks = [(slot_iota == slot_ref[g, pl.ds(s, 1), :]).astype(jnp.bfloat16) for g in range(groups)]
        pick = jnp.concatenate(picks, axis=0) if groups > 1 else picks[0]
        got = jnp.dot(pick, x_ref[s], preferred_element_type=jnp.float32).astype(jnp.bfloat16)
        for g in range(groups):
            put(g, pl.ds(pl.multiple_of(s * cap, 16), cap), got[g * cap:(g + 1) * cap])
        return carry

    lax.fori_loop(0, blk, one, 0)


def first_kernel(cap, sel_ref, slot_ref, x_ref, w_ref, acc_ref, rows_ref):
    def put(g, where, rows):
        rows_ref[g, where, :] = rows

    gather_rows(slot_ref, x_ref, cap, put)
    for g in range(w_ref.shape[0]):
        acc_ref[g] = jnp.dot(rows_ref[g], w_ref[g], preferred_element_type=jnp.float32)


def second_kernel(cap, sel_ref, slot_ref, x_ref, acc_ref, w_ref, v_ref, out_ref, rows_ref):
    def put(g, where, rows):
        rows_ref[g, where, :] = rows

    gather_rows(slot_ref, x_ref, cap, put)
    for g in range(w_ref.shape[0]):
        pre = acc_ref[g] + jnp.dot(rows_ref[g], w_ref[g, -rows_ref.shape[2]:], preferred_element_type=jnp.float32)
        hid = gelu(pre).astype(jnp.bfloat16)
        out = jnp.dot(hid, v_ref[g], preferred_element_type=jnp.float32).astype(jnp.bfloat16)
        out_ref[:, g * cap:(g + 1) * cap] = out.reshape(out_ref.shape[0], cap, out_ref.shape[2])


def combine_kernel(comb_ref, back_ref, part_ref, out_ref):
    routed = jnp.dot(comb_ref[...], back_ref[...], preferred_element_type=jnp.float32)
    out_ref[...] = (part_ref[...] + routed).astype(out_ref.dtype)


def params():
    return pltpu.CompilerParams(dimension_semantics=("arbitrary",), vmem_limit_bytes=VMEM)


def cost(flops, nbytes, trans=0):
    return pl.CostEstimate(flops=int(flops), bytes_accessed=int(nbytes), transcendentals=int(trans))


def once(shape, index):
    return pl.BlockSpec(shape, index, pipeline_mode=pl.Buffered(1))


def expert_first(sel, slots, x_part, w_in, cap):
    groups, srcs, toks = slots.shape
    width, ff, blk = x_part.shape[2], w_in.shape[2], SRC_BLOCK
    return pl.pallas_call(
        functools.partial(first_kernel, cap),
        out_shape=jax.ShapeDtypeStruct((groups, srcs * cap, ff), jnp.float32),
        grid_spec=pltpu.PrefetchScalarGridSpec(
            num_scalar_prefetch=1,
            grid=(srcs // blk,),
            in_specs=[
                pl.BlockSpec((groups, blk, toks), lambda i, sel: (0, i, 0)),
                pl.BlockSpec((blk, toks, width), lambda i, sel: (i, 0, 0)),
                once((groups, width, ff), lambda i, sel: (sel[0], 0, 0)),
            ],
            out_specs=pl.BlockSpec((groups, blk * cap, ff), lambda i, sel: (0, i, 0)),
            scratch_shapes=[pltpu.VMEM((groups, blk * cap, width), jnp.bfloat16)],
        ),
        compiler_params=params(),
        cost_estimate=cost(2 * groups * srcs * cap * width * (ff + toks),
                           srcs * toks * width * 2 + groups * (width * ff * 2 + srcs * cap * ff * 4)),
        name="expert_first",
    )(sel, slots, x_part, w_in)


def expert_second(sel, slots, x_part, acc, w_in, w_out, cap):
    groups, srcs, toks = slots.shape
    width, ff, model, blk = x_part.shape[2], w_out.shape[1], w_out.shape[2], SRC_BLOCK
    cut = w_in.shape[1] - width
    return pl.pallas_call(
        functools.partial(second_kernel, cap),
        out_shape=jax.ShapeDtypeStruct((srcs, groups * cap, model), jnp.bfloat16),
        grid_spec=pltpu.PrefetchScalarGridSpec(
            num_scalar_prefetch=1,
            grid=(srcs // blk,),
            in_specs=[
                pl.BlockSpec((groups, blk, toks), lambda i, sel: (0, i, 0)),
                pl.BlockSpec((blk, toks, width), lambda i, sel: (i, 0, 0)),
                pl.BlockSpec((groups, blk * cap, ff), lambda i, sel: (0, i, 0)),
                once((groups, cut + width, ff), lambda i, sel: (sel[0], 0, 0)),
                once((groups, ff, model), lambda i, sel: (sel[0], 0, 0)),
            ],
            out_specs=pl.BlockSpec((blk, groups * cap, model), lambda i, sel: (i, 0, 0)),
            scratch_shapes=[pltpu.VMEM((groups, blk * cap, width), jnp.bfloat16)],
        ),
        compiler_params=params(),
        cost_estimate=cost(2 * groups * srcs * cap * (width * (ff + toks) + ff * model),
                           srcs * toks * width * 2 + groups * ((width + model) * ff * 2 + srcs * cap * (ff * 4 + model * 2)),
                           groups * srcs * cap * ff),
        name="expert_second",
    )(sel, slots, x_part, acc, w_in, w_out)


def combine(comb, back, part):
    toks, pairs = comb.shape
    model, blk = back.shape[1], COMBINE_BLOCK
    return pl.pallas_call(
        combine_kernel,
        out_shape=jax.ShapeDtypeStruct((toks, model), jnp.bfloat16),
        grid=(model // blk,),
        in_specs=[
            once((toks, pairs), lambda i: (0, 0)),
            pl.BlockSpec((pairs, blk), lambda i: (0, i)),
            pl.BlockSpec((toks, blk), lambda i: (0, i)),
        ],
        out_specs=pl.BlockSpec((toks, blk), lambda i: (0, i)),
        compiler_params=params(),
        cost_estimate=cost(2 * toks * pairs * model, pairs * (toks + model) * 2 + toks * model * 6),
        name="combine",
    )(comb, back, part)


def scatter_kernel(owner, axis, size, rows_ref, out_ref, relay_ref, local_sem, send_sem, hand_sem, land_sem, recv_sem):
    me = lax.axis_index(axis)
    core, partner, chips = owner % 2, owner + 1 - 2 * (owner % 2), size // 2
    stride = next(n for n in range(chips // 3 | 1, 2 * chips) if math.gcd(n, chips) == 1)
    barrier = pltpu.get_barrier_semaphore()

    def remote(src, dst, send, recv, device):
        return pltpu.make_async_remote_copy(
            src_ref=src, dst_ref=dst, send_sem=send, recv_sem=recv,
            device_id={axis: device}, device_id_type=pl.DeviceIdType.MESH)

    def target(k, on_core):
        return 2 * lax.rem(owner // 2 + k * stride, chips) + on_core

    def direct(k):
        dst = target(k, core)
        return remote(rows_ref.at[dst], out_ref, send_sem.at[k], recv_sem, dst)

    def hand(k):
        return remote(rows_ref.at[target(k, 1 - core)], relay_ref.at[k], hand_sem.at[k], land_sem.at[k], partner)

    def forward(k):
        return remote(relay_ref.at[k], out_ref, send_sem.at[k], recv_sem, target(k, 1 - core))

    to_partner = remote(rows_ref.at[partner], out_ref, send_sem.at[0], recv_sem, partner)

    def each(act):
        lax.fori_loop(1, chips, lambda k, c: (act(k), c)[1], 0)

    def tell(device):
        pl.semaphore_signal(barrier, inc=1, device_id={axis: device}, device_id_type=pl.DeviceIdType.MESH)

    @pl.when(me == owner)
    def _():
        mine = pltpu.make_async_copy(rows_ref.at[owner], out_ref, local_sem)
        mine.start()
        pl.semaphore_wait(barrier, size - 1)
        each(lambda k: hand(k).start())
        each(lambda k: direct(k).start())
        to_partner.start()
        each(lambda k: hand(k).wait_send())
        each(lambda k: direct(k).wait_send())
        to_partner.wait_send()
        mine.wait()

    @pl.when(me == partner)
    def _():
        tell(owner)
        pl.semaphore_wait(barrier, size - 2)

        def pass_on(k):
            hand(k).wait_recv()
            forward(k).start()

        each(pass_on)
        each(lambda k: forward(k).wait_send())
        to_partner.wait_recv()

    @pl.when((me != owner) & (me != partner))
    def _():
        tell(owner)
        tell(partner)
        to_partner.wait_recv()


def scatter_from(owner, axis, size, rows):
    chips = size // 2
    return pl.pallas_call(
        functools.partial(scatter_kernel, owner, axis, size),
        out_shape=jax.ShapeDtypeStruct(rows.shape[1:], rows.dtype),
        in_specs=[pl.BlockSpec(memory_space=pl.ANY)],
        out_specs=pl.BlockSpec(memory_space=pl.ANY),
        scratch_shapes=[
            pltpu.VMEM((chips,) + rows.shape[1:], rows.dtype),
            pltpu.SemaphoreType.DMA, pltpu.SemaphoreType.DMA((chips,)), pltpu.SemaphoreType.DMA((chips,)),
            pltpu.SemaphoreType.DMA((chips,)), pltpu.SemaphoreType.DMA,
        ],
        compiler_params=pltpu.CompilerParams(collective_id=0, has_side_effects=True, vmem_limit_bytes=16 * 2 ** 20),
        name="scatter_over",
    )(rows)


def solution(mesh):
    group_size = mesh.shape['ep']

    def local_layer(x_loc, idx_loc, gate_loc, w_in, w_out, shared_in, shared_out):
        tok_rows, top_k = idx_loc.shape
        model = x_loc.shape[1]
        own = w_in.shape[0]
        num_experts = own * group_size
        slot_cap = min(tok_rows, LOAD_MULT * tok_rows * top_k // num_experts)
        cap = BASE_CAP
        over_cap = slot_cap - cap
        cut = model * 5 // 8
        me = lax.axis_index('ep')
        experts = jnp.arange(num_experts, dtype=jnp.int32)

        before = (lax.broadcasted_iota(jnp.int32, (tok_rows, tok_rows), 0)
                  <= lax.broadcasted_iota(jnp.int32, (tok_rows, tok_rows), 1)).astype(jnp.bfloat16)

        def slots_of(hit):
            count = jnp.dot(hit.reshape(-1, tok_rows).astype(jnp.bfloat16), before, preferred_element_type=jnp.float32)
            return jnp.where(hit, count.reshape(hit.shape).astype(jnp.int32) - 1, -1)

        idx_t = idx_loc.T
        count_loc = jnp.sum((idx_t.reshape(1, -1) == experts[:, None]).astype(jnp.int32), axis=1)
        meta = jnp.concatenate([idx_t, jnp.pad(count_loc[None], ((0, 0), (0, tok_rows - num_experts)))], axis=0)
        meta = jnp.pad(meta.astype(jnp.bfloat16), ((0, EXTRA_ROWS - top_k - 1), (0, cut - tok_rows)))
        x_first = lax.all_gather(jnp.concatenate([x_loc[:, :cut], meta], axis=0), 'ep')
        x_second = lax.all_gather(x_loc[:, cut:], 'ep')

        gate_t = gate_loc.astype(jnp.bfloat16).T
        same = idx_t[None] == experts[:, None, None]
        hit_loc = jnp.any(same, axis=1)
        gate_of = jnp.sum(jnp.where(same, gate_t[None], 0).astype(jnp.float32), axis=1).astype(jnp.bfloat16)
        slot_loc = slots_of(hit_loc)

        pick = slot_loc[:, None, :] == jnp.arange(cap, dtype=jnp.int32)[None, :, None]
        comb = jnp.where(pick, gate_of[:, None, :], 0).astype(jnp.bfloat16).reshape(num_experts * cap, tok_rows).T

        def weigh(comb, rows):
            return lax.dot_general(comb, rows, (((0,), (0,)), ((), ())), preferred_element_type=jnp.float32)

        shared_hidden = gelu(jnp.dot(x_loc, shared_in, preferred_element_type=jnp.float32)).astype(jnp.bfloat16)
        shared_val = jnp.dot(shared_hidden, shared_out, preferred_element_type=jnp.float32)
        x_first, shared_val, comb = lax.optimization_barrier((x_first, shared_val, comb))

        idx_all = x_first[:, tok_rows:tok_rows + top_k, :tok_rows].astype(jnp.int32)
        load = jnp.max(x_first[:, tok_rows + top_k, :num_experts].astype(jnp.int32), axis=0)

        def slots_all(expert):
            return slots_of(jnp.any(idx_all == expert, axis=1))

        over = load > cap
        over_rank = jnp.sum((over[None, :] & (experts[None, :] < experts[:, None])).astype(jnp.int32), axis=1)
        num_over = jnp.sum(over.astype(jnp.int32))

        def over_expert(i):
            chosen = over & (over_rank == i)
            return jnp.where(i < num_over, jnp.sum(jnp.where(chosen, experts, 0)), num_experts)

        def over_setup(i):
            expert = over_expert(i)
            mine = expert // own == me
            return expert, mine, jnp.where(mine, expert % own, 0).reshape(1), (slots_all(expert) - cap)[None]

        def over_first(setup, x_part):
            _, mine, sel, slots = setup
            return lax.cond(
                mine, lambda: expert_first(sel, slots, x_part, w_in, over_cap),
                lambda: jnp.zeros((1, group_size * over_cap, w_in.shape[2]), jnp.float32))

        def over_second(setup, x_part, acc):
            _, mine, sel, slots = setup
            return lax.cond(
                mine, lambda: expert_second(sel, slots, x_part, acc, w_in, w_out, over_cap),
                lambda: jnp.zeros((group_size, over_cap, model), jnp.bfloat16))

        base_sel = jnp.zeros((1,), jnp.int32)
        base_slots = jnp.stack([slots_all(me * own + g) for g in range(own)])
        acc = expert_first(base_sel, base_slots, x_first, w_in, cap)
        setups = [over_setup(i) for i in range(HOT_STATIC)]
        over_accs = [over_first(setup, x_first) for setup in setups]
        x_second, acc, over_accs = lax.optimization_barrier((x_second, acc, over_accs))
        out = expert_second(base_sel, base_slots, x_second, acc, w_in, w_out, cap)
        back = lax.all_to_all(out, 'ep', 0, 0, tiled=True).reshape(num_experts * cap, model)
        x_over, over_accs, _ = lax.optimization_barrier((x_second, over_accs, out))
        over_outs = [over_second(s, x_over, a) for s, a in zip(setups, over_accs)]
        over_outs = lax.optimization_barrier(over_outs)

        def over_combine(expert, rows):
            at = jnp.minimum(expert, num_experts - 1)
            slot = lax.dynamic_index_in_dim(slot_loc, at, 0, keepdims=True)
            gate = lax.dynamic_index_in_dim(gate_of, at, 0, keepdims=True)
            pick = (slot - cap == lax.broadcasted_iota(jnp.int32, (over_cap, tok_rows), 0)) & (expert < num_experts)
            return weigh(jnp.where(pick, gate, 0).astype(jnp.bfloat16), rows)

        def scatter(setup, rows):
            owner = jnp.minimum(setup[0], num_experts - 1) // own
            return lax.switch(owner, [functools.partial(scatter_from, d, 'ep', group_size) for d in range(group_size)], rows)

        def spread(rows):
            return lax.psum_scatter(rows.reshape(group_size * over_cap, model), 'ep', scatter_dimension=0, tiled=True)

        rest = [spread(rows) for rows in over_outs[1:]]
        total = shared_val + over_combine(setups[0][0], scatter(setups[0], over_outs[0]))
        for setup, rows in zip(setups[1:], rest):
            total = total + over_combine(setup[0], rows)

        def more(i, total):
            setup = over_setup(i)
            return total + over_combine(setup[0], spread(over_second(setup, x_over, over_first(setup, x_first))))

        total = lax.fori_loop(HOT_STATIC, jnp.maximum(num_over, HOT_STATIC), more, total)
        return combine(comb, back, total)

    tok_spec = P(('dp', 'ep'), None)
    expert_spec = P('ep', None, None)
    whole_spec = P(None, None)
    return jax.shard_map(local_layer, mesh=mesh, in_specs=(tok_spec, tok_spec, tok_spec, expert_spec, expert_spec, whole_spec, whole_spec), out_specs=tok_spec, check_vma=False)
```

```python
import functools
import math

import jax
import jax.numpy as jnp
from jax import lax
from jax.experimental import pallas as pl
from jax.experimental.pallas import tpu as pltpu
from jax.sharding import PartitionSpec as P


LOAD_MULT = 3
BASE_CAP = 48
HOT_STATIC = 2
SRC_BLOCK = 8
COMBINE_BLOCK = 512
EXTRA_ROWS = 16
VMEM = 60 * 2 ** 20


def gelu(z):
    return jax.nn.gelu(z, approximate=True)


def gather_rows(slot_ref, x_ref, cap, put):
    groups, blk, toks = slot_ref.shape
    slot_iota = lax.broadcasted_iota(jnp.int32, (cap, toks), 0)

    def one(s, carry):
        picks = [(slot_iota == slot_ref[g, pl.ds(s, 1), :]).astype(jnp.bfloat16) for g in range(groups)]
        pick = jnp.concatenate(picks, axis=0) if groups > 1 else picks[0]
        got = jnp.dot(pick, x_ref[s], preferred_element_type=jnp.float32).astype(jnp.bfloat16)
        for g in range(groups):
            put(g, pl.ds(pl.multiple_of(s * cap, 16), cap), got[g * cap:(g + 1) * cap])
        return carry

    lax.fori_loop(0, blk, one, 0)


def first_kernel(cap, sel_ref, slot_ref, x_ref, w_ref, acc_ref, rows_ref):
    def put(g, where, rows):
        rows_ref[g, where, :] = rows

    gather_rows(slot_ref, x_ref, cap, put)
    for g in range(w_ref.shape[0]):
        acc_ref[g] = jnp.dot(rows_ref[g], w_ref[g], preferred_element_type=jnp.float32)


def second_kernel(cap, sel_ref, slot_ref, x_ref, acc_ref, w_ref, v_ref, out_ref, rows_ref):
    def put(g, where, rows):
        rows_ref[g, where, :] = rows

    gather_rows(slot_ref, x_ref, cap, put)
    for g in range(w_ref.shape[0]):
        pre = acc_ref[g] + jnp.dot(rows_ref[g], w_ref[g, -rows_ref.shape[2]:], preferred_element_type=jnp.float32)
        hid = gelu(pre).astype(jnp.bfloat16)
        out = jnp.dot(hid, v_ref[g], preferred_element_type=jnp.float32).astype(jnp.bfloat16)
        out_ref[:, g * cap:(g + 1) * cap] = out.reshape(out_ref.shape[0], cap, out_ref.shape[2])


def combine_kernel(*refs):
    part_ref, out_ref = refs[-2:]
    total = part_ref[...]
    for comb_ref, back_ref in zip(refs[:-2:2], refs[1:-2:2]):
        total = total + jnp.dot(comb_ref[...], back_ref[...], preferred_element_type=jnp.float32)
    out_ref[...] = total.astype(out_ref.dtype)


def params():
    return pltpu.CompilerParams(dimension_semantics=("arbitrary",), vmem_limit_bytes=VMEM)


def cost(flops, nbytes, trans=0):
    return pl.CostEstimate(flops=int(flops), bytes_accessed=int(nbytes), transcendentals=int(trans))


def once(shape, index):
    return pl.BlockSpec(shape, index, pipeline_mode=pl.Buffered(1))


def expert_first(sel, slots, x_part, w_in, cap):
    groups, srcs, toks = slots.shape
    width, ff, blk = x_part.shape[2], w_in.shape[2], SRC_BLOCK
    return pl.pallas_call(
        functools.partial(first_kernel, cap),
        out_shape=jax.ShapeDtypeStruct((groups, srcs * cap, ff), jnp.float32),
        grid_spec=pltpu.PrefetchScalarGridSpec(
            num_scalar_prefetch=1,
            grid=(srcs // blk,),
            in_specs=[
                pl.BlockSpec((groups, blk, toks), lambda i, sel: (0, i, 0)),
                pl.BlockSpec((blk, toks, width), lambda i, sel: (i, 0, 0)),
                once((groups, width, ff), lambda i, sel: (sel[0], 0, 0)),
            ],
            out_specs=pl.BlockSpec((groups, blk * cap, ff), lambda i, sel: (0, i, 0)),
            scratch_shapes=[pltpu.VMEM((groups, blk * cap, width), jnp.bfloat16)],
        ),
        compiler_params=params(),
        cost_estimate=cost(2 * groups * srcs * cap * width * (ff + toks),
                           srcs * toks * width * 2 + groups * (width * ff * 2 + srcs * cap * ff * 4)),
        name="expert_first",
    )(sel, slots, x_part, w_in)


def expert_second(sel, slots, x_part, acc, w_in, w_out, cap):
    groups, srcs, toks = slots.shape
    width, ff, model, blk = x_part.shape[2], w_out.shape[1], w_out.shape[2], SRC_BLOCK
    cut = w_in.shape[1] - width
    return pl.pallas_call(
        functools.partial(second_kernel, cap),
        out_shape=jax.ShapeDtypeStruct((srcs, groups * cap, model), jnp.bfloat16),
        grid_spec=pltpu.PrefetchScalarGridSpec(
            num_scalar_prefetch=1,
            grid=(srcs // blk,),
            in_specs=[
                pl.BlockSpec((groups, blk, toks), lambda i, sel: (0, i, 0)),
                pl.BlockSpec((blk, toks, width), lambda i, sel: (i, 0, 0)),
                pl.BlockSpec((groups, blk * cap, ff), lambda i, sel: (0, i, 0)),
                once((groups, cut + width, ff), lambda i, sel: (sel[0], 0, 0)),
                once((groups, ff, model), lambda i, sel: (sel[0], 0, 0)),
            ],
            out_specs=pl.BlockSpec((blk, groups * cap, model), lambda i, sel: (i, 0, 0)),
            scratch_shapes=[pltpu.VMEM((groups, blk * cap, width), jnp.bfloat16)],
        ),
        compiler_params=params(),
        cost_estimate=cost(2 * groups * srcs * cap * (width * (ff + toks) + ff * model),
                           srcs * toks * width * 2 + groups * ((width + model) * ff * 2 + srcs * cap * (ff * 4 + model * 2)),
                           groups * srcs * cap * ff),
        name="expert_second",
    )(sel, slots, x_part, acc, w_in, w_out)


def combine(pairs, part):
    toks, model = part.shape
    blk = COMBINE_BLOCK
    depth = sum(rows.shape[0] for _, rows in pairs)
    specs = []
    for comb, rows in pairs:
        specs += [once(comb.shape, lambda i: (0, 0)), pl.BlockSpec((rows.shape[0], blk), lambda i: (0, i))]
    return pl.pallas_call(
        combine_kernel,
        out_shape=jax.ShapeDtypeStruct((toks, model), jnp.bfloat16),
        grid=(model // blk,),
        in_specs=specs + [pl.BlockSpec((toks, blk), lambda i: (0, i))],
        out_specs=pl.BlockSpec((toks, blk), lambda i: (0, i)),
        compiler_params=params(),
        cost_estimate=cost(2 * toks * depth * model, depth * (toks + model) * 2 + toks * model * 6),
        name="combine",
    )(*[ref for pair in pairs for ref in pair], part)


def scatter_kernel(owner, axis, size, rows_ref, out_ref, relay_ref, local_sem, send_sem, hand_sem, land_sem, recv_sem):
    me = lax.axis_index(axis)
    core, partner, chips = owner % 2, owner + 1 - 2 * (owner % 2), size // 2
    stride = next(n for n in range(chips // 3 | 1, 2 * chips) if math.gcd(n, chips) == 1)
    barrier = pltpu.get_barrier_semaphore()

    def remote(src, dst, send, recv, device):
        return pltpu.make_async_remote_copy(
            src_ref=src, dst_ref=dst, send_sem=send, recv_sem=recv,
            device_id={axis: device}, device_id_type=pl.DeviceIdType.MESH)

    def target(k, on_core):
        return 2 * lax.rem(owner // 2 + k * stride, chips) + on_core

    def direct(k):
        dst = target(k, core)
        return remote(rows_ref.at[dst], out_ref, send_sem.at[k], recv_sem, dst)

    def hand(k):
        return remote(rows_ref.at[target(k, 1 - core)], relay_ref.at[k], hand_sem.at[k], land_sem.at[k], partner)

    def forward(k):
        return remote(relay_ref.at[k], out_ref, send_sem.at[k], recv_sem, target(k, 1 - core))

    to_partner = remote(rows_ref.at[partner], out_ref, send_sem.at[0], recv_sem, partner)

    def each(act):
        lax.fori_loop(1, chips, lambda k, c: (act(k), c)[1], 0)

    def tell(device):
        pl.semaphore_signal(barrier, inc=1, device_id={axis: device}, device_id_type=pl.DeviceIdType.MESH)

    @pl.when(me == owner)
    def _():
        mine = pltpu.make_async_copy(rows_ref.at[owner], out_ref, local_sem)
        mine.start()
        pl.semaphore_wait(barrier, size - 1)
        each(lambda k: hand(k).start())
        each(lambda k: direct(k).start())
        to_partner.start()
        each(lambda k: hand(k).wait_send())
        each(lambda k: direct(k).wait_send())
        to_partner.wait_send()
        mine.wait()

    @pl.when(me == partner)
    def _():
        tell(owner)
        pl.semaphore_wait(barrier, size - 2)

        def pass_on(k):
            hand(k).wait_recv()
            forward(k).start()

        each(pass_on)
        each(lambda k: forward(k).wait_send())
        to_partner.wait_recv()

    @pl.when((me != owner) & (me != partner))
    def _():
        tell(owner)
        tell(partner)
        to_partner.wait_recv()


def scatter_from(owner, axis, size, rows):
    chips = size // 2
    return pl.pallas_call(
        functools.partial(scatter_kernel, owner, axis, size),
        out_shape=jax.ShapeDtypeStruct(rows.shape[1:], rows.dtype),
        in_specs=[pl.BlockSpec(memory_space=pl.ANY)],
        out_specs=pl.BlockSpec(memory_space=pl.ANY),
        scratch_shapes=[
            pltpu.VMEM((chips,) + rows.shape[1:], rows.dtype),
            pltpu.SemaphoreType.DMA, pltpu.SemaphoreType.DMA((chips,)), pltpu.SemaphoreType.DMA((chips,)),
            pltpu.SemaphoreType.DMA((chips,)), pltpu.SemaphoreType.DMA,
        ],
        compiler_params=pltpu.CompilerParams(collective_id=0, has_side_effects=True, vmem_limit_bytes=16 * 2 ** 20),
        name="scatter_over",
    )(rows)


def solution(mesh):
    group_size = mesh.shape['ep']

    def local_layer(x_loc, idx_loc, gate_loc, w_in, w_out, shared_in, shared_out):
        tok_rows, top_k = idx_loc.shape
        model = x_loc.shape[1]
        own = w_in.shape[0]
        num_experts = own * group_size
        slot_cap = min(tok_rows, LOAD_MULT * tok_rows * top_k // num_experts)
        cap = BASE_CAP
        over_cap = slot_cap - cap
        cut = model * 5 // 8
        me = lax.axis_index('ep')
        experts = jnp.arange(num_experts, dtype=jnp.int32)

        before = (lax.broadcasted_iota(jnp.int32, (tok_rows, tok_rows), 0)
                  <= lax.broadcasted_iota(jnp.int32, (tok_rows, tok_rows), 1)).astype(jnp.bfloat16)

        def slots_of(hit):
            count = jnp.dot(hit.reshape(-1, tok_rows).astype(jnp.bfloat16), before, preferred_element_type=jnp.float32)
            return jnp.where(hit, count.reshape(hit.shape).astype(jnp.int32) - 1, -1)

        idx_t = idx_loc.T
        count_loc = jnp.sum((idx_t.reshape(1, -1) == experts[:, None]).astype(jnp.int32), axis=1)
        meta = jnp.concatenate([idx_t, jnp.pad(count_loc[None], ((0, 0), (0, tok_rows - num_experts)))], axis=0)
        meta = jnp.pad(meta.astype(jnp.bfloat16), ((0, EXTRA_ROWS - top_k - 1), (0, cut - tok_rows)))
        x_first = lax.all_gather(jnp.concatenate([x_loc[:, :cut], meta], axis=0), 'ep')
        x_second = lax.all_gather(x_loc[:, cut:], 'ep')

        gate_t = gate_loc.astype(jnp.bfloat16).T
        same = idx_t[None] == experts[:, None, None]
        hit_loc = jnp.any(same, axis=1)
        gate_of = jnp.sum(jnp.where(same, gate_t[None], 0).astype(jnp.float32), axis=1).astype(jnp.bfloat16)
        slot_loc = slots_of(hit_loc)

        pick = slot_loc[:, None, :] == jnp.arange(cap, dtype=jnp.int32)[None, :, None]
        comb = jnp.where(pick, gate_of[:, None, :], 0).astype(jnp.bfloat16).reshape(num_experts * cap, tok_rows).T

        shared_hidden = gelu(jnp.dot(x_loc, shared_in, preferred_element_type=jnp.float32)).astype(jnp.bfloat16)
        shared_val = jnp.dot(shared_hidden, shared_out, preferred_element_type=jnp.float32)
        x_first, shared_val, comb = lax.optimization_barrier((x_first, shared_val, comb))

        idx_all = x_first[:, tok_rows:tok_rows + top_k, :tok_rows].astype(jnp.int32)
        load = jnp.max(x_first[:, tok_rows + top_k, :num_experts].astype(jnp.int32), axis=0)

        def slots_all(expert):
            return slots_of(jnp.any(idx_all == expert, axis=1))

        over = load > cap
        over_rank = jnp.sum((over[None, :] & (experts[None, :] < experts[:, None])).astype(jnp.int32), axis=1)
        num_over = jnp.sum(over.astype(jnp.int32))

        def over_expert(i):
            chosen = over & (over_rank == i)
            return jnp.where(i < num_over, jnp.sum(jnp.where(chosen, experts, 0)), num_experts)

        def over_setup(i):
            expert = over_expert(i)
            mine = expert // own == me
            return expert, mine, jnp.where(mine, expert % own, 0).reshape(1), (slots_all(expert) - cap)[None]

        def over_first(setup, x_part):
            _, mine, sel, slots = setup
            return lax.cond(
                mine, lambda: expert_first(sel, slots, x_part, w_in, over_cap),
                lambda: jnp.zeros((1, group_size * over_cap, w_in.shape[2]), jnp.float32))

        def over_second(setup, x_part, acc):
            _, mine, sel, slots = setup
            return lax.cond(
                mine, lambda: expert_second(sel, slots, x_part, acc, w_in, w_out, over_cap),
                lambda: jnp.zeros((group_size, over_cap, model), jnp.bfloat16))

        base_sel = jnp.zeros((1,), jnp.int32)
        base_slots = jnp.stack([slots_all(me * own + g) for g in range(own)])
        acc = expert_first(base_sel, base_slots, x_first, w_in, cap)
        setups = [over_setup(i) for i in range(HOT_STATIC)]
        over_accs = [over_first(setup, x_first) for setup in setups]
        x_second, acc, over_accs = lax.optimization_barrier((x_second, acc, over_accs))
        out = expert_second(base_sel, base_slots, x_second, acc, w_in, w_out, cap)
        back = lax.all_to_all(out, 'ep', 0, 0, tiled=True).reshape(num_experts * cap, model)
        x_over, over_accs, _ = lax.optimization_barrier((x_second, over_accs, out))
        over_outs = [over_second(s, x_over, a) for s, a in zip(setups, over_accs)]
        over_outs = lax.optimization_barrier(over_outs)

        def over_table(expert):
            at = jnp.minimum(expert, num_experts - 1)
            slot = lax.dynamic_index_in_dim(slot_loc, at, 0, keepdims=True)
            gate = lax.dynamic_index_in_dim(gate_of, at, 0, keepdims=True)
            pick = (slot - cap == lax.broadcasted_iota(jnp.int32, (over_cap, tok_rows), 0)) & (expert < num_experts)
            return jnp.where(pick, gate, 0).astype(jnp.bfloat16).T

        def scatter(setup, rows):
            owner = jnp.minimum(setup[0], num_experts - 1) // own
            return lax.switch(owner, [functools.partial(scatter_from, d, 'ep', group_size) for d in range(group_size)], rows)

        def spread(rows):
            return lax.psum_scatter(rows.reshape(group_size * over_cap, model), 'ep', scatter_dimension=0, tiled=True)

        rest = [spread(rows) for rows in over_outs[1:]]
        tables = [over_table(setup[0]) for setup in setups]

        def more(i, total):
            setup = over_setup(i)
            rows = spread(over_second(setup, x_over, over_first(setup, x_first)))
            return total + jnp.dot(over_table(setup[0]), rows, preferred_element_type=jnp.float32)

        first, tables = lax.optimization_barrier((over_outs[0], tables))
        sent = scatter(setups[0], first)
        sent, rest, total = lax.optimization_barrier((sent, rest, shared_val))
        total = lax.fori_loop(HOT_STATIC, jnp.maximum(num_over, HOT_STATIC), more, total)
        return combine([(comb, back)] + list(zip(tables, [sent] + rest)), total)

    tok_spec = P(('dp', 'ep'), None)
    expert_spec = P('ep', None, None)
    whole_spec = P(None, None)
    return jax.shard_map(local_layer, mesh=mesh, in_specs=(tok_spec, tok_spec, tok_spec, expert_spec, expert_spec, whole_spec, whole_spec), out_specs=tok_spec, check_vma=False)
```
